32 devices in a mesh: dp: 4 (over x, y), tp: 8 (over z, core).
Axes of the slice: x: 2, y: 2, z: 4, core: 2. Of those that a mesh axis runs over, the one named last changes fastest.
Arguments:
- x_in: bfloat16 [8, 2048, 2048], P('dp'), parts along dimension 0
- start_pos: int32 [8], P('dp'), parts along dimension 0
- kv_state: float32 [8, 8, 256, 512], P('dp', 'tp'), parts along dimension 0
- ln1_gain: float32 [2048], replicated
- ln1_bias: float32 [2048], replicated
- w_q: bfloat16 [2048, 2048], P(None, 'tp')
- w_k: bfloat16 [2048, 2048], P(None, 'tp')
- w_v: bfloat16 [2048, 4096], P(None, 'tp')
- w_g: bfloat16 [2048, 4096], P(None, 'tp')
- w_o: bfloat16 [4096, 2048], P('tp')
- ln2_gain: float32 [2048], replicated
- ln2_bias: float32 [2048], replicated
- w_up: bfloat16 [2048, 4096], P(None, 'tp')
- w_down: bfloat16 [4096, 2048], P('tp')
Outputs:
- output 1: bfloat16 [8, 2048, 2048], P('dp'), parts along dimension 0
- output 2: float32 [8, 8, 256, 512], P('dp', 'tp'), parts along dimension 0
There are 4 independent parts. The reference program is written for one: setup_inputs(seed, part) draws one part's arguments, and reference() takes and returns one part's arrays. A program takes and returns all parts, laid end to end along the dimension named above; an argument that names none is the same for every part.
All inputs are finite; a program needn't handle non-finite values.
Results may differ from the reference program's by a relative error of at most 0.0145129.
Values are sent between devices in bfloat16 or wider.
A program may use at most 1 GiB of HBM per device.

```python
import jax
import jax.numpy as jnp
from jax import lax

BATCH_SEQS = 2
CHUNK_LEN = 2048
D_MODEL = 2048
NUM_HEADS = 8
FFN_DIM = 4096
POS_LIMIT = 4096

KEY_DIM = D_MODEL // NUM_HEADS
VAL_DIM = 2 * KEY_DIM
HALF_DIM = KEY_DIM // 2
NORM_EPS = 1e-5
GROUP_EPS = 1e-6
ROPE_BASE = 10000.0


def head_log_decay():
    head_ids = jnp.arange(NUM_HEADS).astype(jnp.float32)
    return jnp.log1p(-jnp.exp2(-5.0 - head_ids))


def setup_inputs(seed: int = 0, part: int = 0) -> dict:
    base_key = jax.random.key(seed)
    weight_keys = jax.random.split(base_key, 12)
    part_keys = jax.random.split(jax.random.fold_in(weight_keys[11], part), 3)

    def normal_weight(key_index, arr_shape, fan_in):
        raw_draw = jax.random.normal(weight_keys[key_index], arr_shape, jnp.float32)
        return (raw_draw * fan_in ** -0.5).astype(jnp.bfloat16)

    x_in = jax.random.normal(part_keys[0], (BATCH_SEQS, CHUNK_LEN, D_MODEL), jnp.float32).astype(jnp.bfloat16)
    start_pos = jax.random.randint(part_keys[1], (BATCH_SEQS,), 64, POS_LIMIT, dtype=jnp.int32)
    log_gamma = head_log_decay()
    decayed_var = jnp.expm1(2.0 * start_pos.astype(jnp.float32)[:, None] * log_gamma[None, :]) / jnp.expm1(2.0 * log_gamma)[None, :]
    state_draw = jax.random.normal(part_keys[2], (BATCH_SEQS, NUM_HEADS, KEY_DIM, VAL_DIM), jnp.float32)
    kv_state = state_draw * jnp.sqrt(decayed_var / KEY_DIM)[:, :, None, None]
    return {
        'x_in': x_in,
        'start_pos': start_pos,
        'kv_state': kv_state,
        'ln1_gain': 1.0 + 0.3 * jax.random.normal(weight_keys[0], (D_MODEL,), jnp.float32),
        'ln1_bias': 0.3 * jax.random.normal(weight_keys[1], (D_MODEL,), jnp.float32),
        'w_q': normal_weight(2, (D_MODEL, D_MODEL), D_MODEL),
        'w_k': normal_weight(3, (D_MODEL, D_MODEL), D_MODEL),
        'w_v': normal_weight(4, (D_MODEL, 2 * D_MODEL), D_MODEL),
        'w_g': normal_weight(5, (D_MODEL, 2 * D_MODEL), D_MODEL),
        'w_o': normal_weight(6, (2 * D_MODEL, D_MODEL), 2 * D_MODEL),
        'ln2_gain': 1.0 + 0.3 * jax.random.normal(weight_keys[7], (D_MODEL,), jnp.float32),
        'ln2_bias': 0.3 * jax.random.normal(weight_keys[8], (D_MODEL,), jnp.float32),
        'w_up': normal_weight(9, (D_MODEL, FFN_DIM), D_MODEL),
        'w_down': normal_weight(10, (FFN_DIM, D_MODEL), FFN_DIM),
    }


def layer_norm(x_f32, norm_gain, norm_bias):
    row_mean = jnp.mean(x_f32, axis=-1, keepdims=True)
    centered = x_f32 - row_mean
    variance = jnp.mean(centered * centered, axis=-1, keepdims=True)
    return centered * lax.rsqrt(variance + NORM_EPS) * norm_gain + norm_bias


def rotate_half(head_vecs, cos_t, sin_t):
    first_half = head_vecs[..., :HALF_DIM]
    second_half = head_vecs[..., HALF_DIM:]
    return jnp.concatenate([first_half * cos_t - second_half * sin_t, second_half * cos_t + first_half * sin_t], axis=-1)


def reference(x_in, start_pos, kv_state, ln1_gain, ln1_bias, w_q, w_k, w_v, w_g, w_o, ln2_gain, ln2_bias, w_up, w_down):
    log_gamma = head_log_decay()
    step_ids = jnp.arange(CHUNK_LEN)
    step_gap = step_ids[:, None] - step_ids[None, :]
    inner_decay = jnp.where(step_gap[None] >= 0, jnp.exp(jnp.maximum(step_gap, 0).astype(jnp.float32)[None] * log_gamma[:, None, None]), 0.0)
    query_decay = jnp.exp((step_ids + 1).astype(jnp.float32)[:, None] * log_gamma[None, :])
    key_decay = jnp.exp((CHUNK_LEN - 1 - step_ids).astype(jnp.float32)[:, None] * log_gamma[None, :])
    state_decay = jnp.exp(CHUNK_LEN * log_gamma)
    inv_freq = jnp.power(ROPE_BASE, -jnp.arange(HALF_DIM).astype(jnp.float32) / HALF_DIM)

    def one_sequence(packed):
        tokens, first_pos, old_state = packed
        x_f32 = tokens.astype(jnp.float32)
        h_one = layer_norm(x_f32, ln1_gain, ln1_bias).astype(jnp.bfloat16)
        angles = (first_pos + step_ids).astype(jnp.float32)[:, None] * inv_freq[None, :]
        cos_t = jnp.cos(angles)[:, None, :]
        sin_t = jnp.sin(angles)[:, None, :]
        q_raw = jnp.dot(h_one, w_q, preferred_element_type=jnp.float32).reshape(CHUNK_LEN, NUM_HEADS, KEY_DIM)
        k_raw = jnp.dot(h_one, w_k, preferred_element_type=jnp.float32).reshape(CHUNK_LEN, NUM_HEADS, KEY_DIM)
        queries = rotate_half(q_raw, cos_t, sin_t).astype(jnp.bfloat16).astype(jnp.float32)
        keys = (rotate_half(k_raw, cos_t, sin_t) * KEY_DIM ** -0.5).astype(jnp.bfloat16).astype(jnp.float32)
        values = jnp.dot(h_one, w_v, preferred_element_type=jnp.float32).astype(jnp.bfloat16).astype(jnp.float32).reshape(CHUNK_LEN, NUM_HEADS, VAL_DIM)
        gates = jnp.dot(h_one, w_g, preferred_element_type=jnp.float32).reshape(CHUNK_LEN, NUM_HEADS, VAL_DIM)
        scores = jnp.einsum('chk,jhk->hcj', queries, keys) * inner_decay
        retained = jnp.einsum('hcj,jhe->che', scores, values) + jnp.einsum('chk,hke->che', queries, old_state) * query_decay[:, :, None]
        row_mean = jnp.mean(retained, axis=-1, keepdims=True)
        centered = retained - row_mean
        variance = jnp.mean(centered * centered, axis=-1, keepdims=True)
        normed = centered * lax.rsqrt(variance + GROUP_EPS)
        mixed = (jax.nn.silu(gates) * normed).astype(jnp.bfloat16).reshape(CHUNK_LEN, 2 * D_MODEL)
        attn_out = jnp.dot(mixed, w_o, preferred_element_type=jnp.float32).astype(jnp.bfloat16)
        x_mid = (x_f32 + attn_out.astype(jnp.float32)).astype(jnp.bfloat16)
        h_two = layer_norm(x_mid.astype(jnp.float32), ln2_gain, ln2_bias).astype(jnp.bfloat16)
        activated = jax.nn.gelu(jnp.dot(h_two, w_up, preferred_element_type=jnp.float32), approximate=False).astype(jnp.bfloat16)
        ffn_out = jnp.dot(activated, w_down, preferred_element_type=jnp.float32).astype(jnp.bfloat16)
        x_out = (x_mid.astype(jnp.float32) + ffn_out.astype(jnp.float32)).astype(jnp.bfloat16)
        new_state = state_decay[:, None, None] * old_state + jnp.einsum('jhk,jhe->hke', keys * key_decay[:, :, None], values)
        return x_out, new_state

    x_out, state_out = lax.map(one_sequence, (x_in, start_pos, kv_state))
    return (x_out, state_out)
```

```python
import functools

import jax
import jax.numpy as jnp
from jax import lax
from jax.experimental import pallas as pl
from jax.experimental.pallas import tpu as pltpu
from jax.sharding import PartitionSpec as P

NORM_EPS = 1e-5
GROUP_EPS = 1e-6
ROPE_BASE = 10000.0
CHUNK = 256
BLOCKS = 4
HALVES = 2
CORES = 2
F32 = jnp.float32
BF16 = jnp.bfloat16


def normalize(x_f32, gain, bias):
    row_mean = jnp.mean(x_f32, axis=-1, keepdims=True)
    centered = x_f32 - row_mean
    variance = jnp.mean(centered * centered, axis=-1, keepdims=True)
    return centered * lax.rsqrt(variance + NORM_EPS) * gain + bias


def attention_kernel(chunk, x_ref, state_in_ref, gain_ref, bias_ref, wq_ref, wk_ref, wv_ref, wg_ref, wo_ref, base_ref, table_ref, decay_ref, edge_ref, u_ref, state_ref):
    step = pl.program_id(1)
    key_dim = wq_ref.shape[1]
    half = key_dim // 2

    @pl.when(step == 0)
    def _():
        state_ref[...] = state_in_ref[...]

    h = normalize(x_ref[0].astype(F32), gain_ref[...], bias_ref[...]).astype(BF16)
    q_raw = jnp.dot(h, wq_ref[...], preferred_element_type=F32)
    k_raw = jnp.dot(h, wk_ref[...], preferred_element_type=F32)
    v_all = jnp.dot(h, wv_ref[...], preferred_element_type=F32).astype(BF16)
    g_all = jnp.dot(h, wg_ref[...], preferred_element_type=F32)
    cos_lo, sin_lo = table_ref[0], table_ref[1]
    mixed = []
    for sub in range(h.shape[0] // chunk):
        rows = slice(sub * chunk, (sub + 1) * chunk)
        cos_hi, sin_hi = base_ref[0, 0, sub, 0:1, :], base_ref[0, 0, sub, 1:2, :]
        cos_t = cos_hi * cos_lo - sin_hi * sin_lo
        sin_t = sin_hi * cos_lo + cos_hi * sin_lo

        def rotate(raw):
            first, second = raw[rows, :half], raw[rows, half:]
            return jnp.concatenate([first * cos_t - second * sin_t, second * cos_t + first * sin_t], axis=-1)

        queries = rotate(q_raw).astype(BF16)
        keys = (rotate(k_raw) * key_dim ** -0.5).astype(BF16)
        values = v_all[rows]
        state = state_ref[0, 0]
        scores = lax.dot_general(queries, keys, (((1,), (1,)), ((), ())), preferred_element_type=F32) * decay_ref[...]
        retained = jnp.dot(scores.astype(BF16), values, preferred_element_type=F32)
        retained += jnp.dot(queries, state.astype(BF16), preferred_element_type=F32) * edge_ref[:, 0:1]
        keys_decayed = (keys.astype(F32) * edge_ref[:, 1:2]).astype(BF16)
        grown = lax.dot_general(keys_decayed, values, (((0,), (0,)), ((), ())), preferred_element_type=F32)
        state_ref[0, 0] = state * edge_ref[0:1, 2:3] + grown
        row_mean = jnp.mean(retained, axis=-1, keepdims=True)
        centered = retained - row_mean
        variance = jnp.mean(centered * centered, axis=-1, keepdims=True)
        normed = centered * lax.rsqrt(variance + GROUP_EPS)
        mixed.append((jax.nn.silu(g_all[rows]) * normed).astype(BF16))
    u_ref[0] = jnp.dot(jnp.concatenate(mixed, axis=0), wo_ref[...], preferred_element_type=F32).astype(BF16)


def attention_block(block, rows, x_in, state, gain, bias, w_q, w_k, w_v, w_g, w_o, base, table, decay, edge):
    seqs, _, d_model = x_in.shape
    key_dim, val_dim = state.shape[2:]
    chunk = decay.shape[0]
    step_rows = min(2 * chunk, rows)
    steps = rows // step_rows
    subs = step_rows // chunk
    whole = lambda a: pl.BlockSpec(a.shape, lambda b, i: (0,) * a.ndim)
    state_spec = pl.BlockSpec((1, 1, key_dim, val_dim), lambda b, i: (b, 0, 0, 0))
    tokens = seqs * rows
    flops = 2 * tokens * (d_model * (2 * key_dim + 2 * val_dim) + val_dim * d_model + chunk * (key_dim + val_dim) + 2 * key_dim * val_dim)
    return pl.pallas_call(
        functools.partial(attention_kernel, chunk),
        grid=(seqs, steps),
        in_specs=[
            pl.BlockSpec((1, step_rows, d_model), lambda b, i: (b, i + block * steps, 0)),
            state_spec,
            whole(gain), whole(bias), whole(w_q), whole(w_k), whole(w_v), whole(w_g), whole(w_o),
            pl.BlockSpec((1, 1, subs) + base.shape[3:], lambda b, i: (b, i + block * steps, 0, 0, 0)),
            whole(table), whole(decay), whole(edge),
        ],
        out_specs=[pl.BlockSpec((1, step_rows, d_model), lambda b, i: (b, i, 0)), state_spec],
        out_shape=[jax.ShapeDtypeStruct((seqs, rows, d_model), BF16), jax.ShapeDtypeStruct(state.shape, F32)],
        compiler_params=pltpu.CompilerParams(vmem_limit_bytes=58 * 2 ** 20),
        cost_estimate=pl.CostEstimate(flops=flops, bytes_accessed=2 * 2 * tokens * d_model + 10 * 2 ** 20, transcendentals=0),
        name="attention",
    )(x_in, state, gain, bias, w_q, w_k, w_v, w_g, w_o, base, table, decay, edge)


def ffn_kernel(x_ref, gain_ref, bias_ref, up_ref, down_ref, out_ref, h_ref, acc_ref):
    step = pl.program_id(0)
    quarters, depth, width = up_ref.shape[0], up_ref.shape[3], up_ref.shape[4]

    @pl.when(step == 0)
    def _():
        h_ref[...] = normalize(x_ref[...].astype(F32), gain_ref[...], bias_ref[...]).astype(BF16)
        acc_ref[...] = jnp.zeros_like(acc_ref)

    pre = jnp.zeros((h_ref.shape[0], width), F32)
    for q in range(quarters):
        pre += jnp.dot(h_ref[:, q * depth:(q + 1) * depth], up_ref[q, 0, 0], preferred_element_type=F32)
    act = (0.5 * pre * (1.0 + lax.erf(pre * 0.5 ** 0.5))).astype(BF16)
    for q in range(quarters):
        cols = slice(q * depth, (q + 1) * depth)
        acc_ref[:, cols] += jnp.dot(act, down_ref[q, 0, 0], preferred_element_type=F32)

    @pl.when(step == pl.num_programs(0) - 1)
    def _():
        f = acc_ref[...].astype(BF16).astype(F32)
        out_ref[...] = (x_ref[...].astype(F32) + f).astype(BF16)


def feed_forward(x_mid, gain, bias, weights):
    rows, d_model = x_mid.shape
    quarters, shards, _, depth, width = weights.shape
    whole = lambda a: pl.BlockSpec(a.shape, lambda s: (0,) * a.ndim)
    half_spec = lambda which: pl.BlockSpec((quarters, 1, 1, depth, width), lambda s: (0, s, which, 0, 0))
    return pl.pallas_call(
        ffn_kernel,
        grid=(shards,),
        in_specs=[whole(x_mid), whole(gain), whole(bias), half_spec(0), half_spec(1)],
        out_specs=pl.BlockSpec(x_mid.shape, lambda s: (0, 0)),
        out_shape=jax.ShapeDtypeStruct(x_mid.shape, BF16),
        scratch_shapes=[pltpu.VMEM(x_mid.shape, BF16), pltpu.VMEM(x_mid.shape, F32)],
        compiler_params=pltpu.CompilerParams(vmem_limit_bytes=58 * 2 ** 20),
        cost_estimate=pl.CostEstimate(flops=4 * rows * d_model * shards * width, bytes_accessed=2 * weights.size, transcendentals=0),
        name="ffn",
    )(x_mid, gain, bias, weights, weights)


def add_bf16(*terms):
    return sum(t.astype(F32) for t in terms).astype(BF16)


def line_pairs(chips, shift, first, last):
    return [(j * CORES + c, (j + shift) * CORES + c) for j in range(first, last + 1) for c in range(CORES)]


def reduce_scatter_line(own, chip, chips):
    def piece(k):
        return lax.dynamic_index_in_dim(own, lax.rem(k + chips, chips), 0, keepdims=False)

    right = left = None
    for t in range(1, chips):
        send_right, send_left = piece(chip - t), piece(chip + t)
        if t > 1:
            send_right, send_left = add_bf16(send_right, right), add_bf16(send_left, left)
        right = lax.ppermute(send_right, 'tp', line_pairs(chips, 1, 0, t - 1))
        left = lax.ppermute(send_left, 'tp', line_pairs(chips, -1, chips - t, chips - 1))
    return piece(chip), right, left


def all_gather_line(own, chip, chips):
    right = left = own
    from_left, from_right = [], []
    for t in range(1, chips):
        right = lax.ppermute(right, 'tp', line_pairs(chips, 1, t - 1, chips - 2))
        left = lax.ppermute(left, 'tp', line_pairs(chips, -1, 1, chips - t))
        from_left.append(right)
        from_right.append(left)
    pieces = [own]
    for d in range(1, chips):
        pieces.append(from_left[d - 1] + from_right[chips - d - 1])
    return pieces


def solution(mesh):
    groups, members = mesh.shape['dp'], mesh.shape['tp']
    chips = members // CORES

    def local_layer(x_in, start_pos, kv_state, ln1_gain, ln1_bias, w_q, w_k, w_v, w_g, w_o, ln2_gain, ln2_bias, w_up, w_down):
        seqs, chunk_len, d_model = x_in.shape
        key_dim = kv_state.shape[2]
        half = key_dim // 2
        me, group = lax.axis_index('tp'), lax.axis_index('dp')
        chip, core = me // CORES, lax.rem(me, CORES)
        partner = [(t, t ^ 1) for t in range(members)]

        depth = d_model // groups
        up_piece = lax.dynamic_slice_in_dim(w_up, group * depth, depth, 0)
        down_piece = lax.dynamic_slice_in_dim(w_down, group * depth, depth, 1)
        weights = lax.all_gather(jnp.stack([up_piece, down_piece]), ('dp', 'tp'))
        weights = weights.reshape((groups, members) + weights.shape[1:])

        chunk = min(CHUNK, chunk_len // BLOCKS)
        log_gamma = jnp.log1p(-jnp.exp2(-5.0 - me.astype(F32)))
        ids = jnp.arange(chunk)
        gap = ids[:, None] - ids[None, :]
        decay = jnp.where(gap >= 0, jnp.exp(jnp.maximum(gap, 0).astype(F32) * log_gamma), 0.0)
        edge = jnp.stack([jnp.exp((ids + 1).astype(F32) * log_gamma), jnp.exp((chunk - 1 - ids).astype(F32) * log_gamma), jnp.full((chunk,), jnp.exp(chunk * log_gamma))], axis=1)
        edge = jnp.pad(edge, ((0, 0), (0, 128 - edge.shape[1])))
        inv_freq = jnp.power(ROPE_BASE, -jnp.arange(half).astype(F32) / half)
        low = ids.astype(F32)[:, None] * inv_freq[None, :]
        table = jnp.stack([jnp.cos(low), jnp.sin(low)])
        rows = chunk_len // BLOCKS
        subs = min(2 * chunk, rows) // chunk
        high = (start_pos[:, None] + jnp.arange(chunk_len // chunk)[None, :] * chunk).astype(F32)[:, :, None] * inv_freq
        base = jnp.stack([jnp.cos(high), jnp.sin(high)], axis=2)
        base = base.reshape(seqs, chunk_len // chunk // subs, subs, 2, half)

        gain1, bias1, gain2, bias2 = (a[None, :] for a in (ln1_gain, ln1_bias, ln2_gain, ln2_bias))
        state = kv_state
        share = rows // chips
        mids = []
        for block in range(BLOCKS):
            part, state = attention_block(block, rows, x_in, state, gain1, bias1, w_q, w_k, w_v, w_g, w_o, base, table, decay, edge)
            other = lax.ppermute(lax.dynamic_index_in_dim(part, 1 - core, 0, keepdims=False), 'tp', partner)
            own = add_bf16(lax.dynamic_index_in_dim(part, core, 0, keepdims=False), other)
            u = add_bf16(*reduce_scatter_line(own.reshape(chips, share, d_model), chip, chips))
            x_own = lax.dynamic_slice(x_in, (core, block * rows + chip * share, 0), (1, share, d_model))[0]
            mids.append(add_bf16(x_own, u))

        per_half = BLOCKS // HALVES
        outs = []
        for half_id in range(HALVES):
            x_mid = jnp.concatenate(mids[half_id * per_half:(half_id + 1) * per_half], axis=0)
            x_new = feed_forward(x_mid, gain2, bias2, weights)
            pieces = all_gather_line(x_new, chip, chips)
            mine = jnp.zeros((chips,) + x_new.shape, BF16)
            for d in range(chips):
                mine = lax.dynamic_update_index_in_dim(mine, pieces[d], lax.rem(chip - d + chips, chips), 0)
            mine = mine.reshape(chips, per_half, share, d_model).swapaxes(0, 1).reshape(per_half * rows, d_model)
            other = lax.ppermute(mine, 'tp', partner)
            outs.append(jnp.where(core == 0, jnp.stack([mine, other]), jnp.stack([other, mine])))
        return jnp.concatenate(outs, axis=1), state

    in_specs = (P('dp', None, None), P('dp'), P('dp', 'tp', None, None), P(), P(), P(None, 'tp'), P(None, 'tp'), P(None, 'tp'), P(None, 'tp'), P('tp', None), P(), P(), P(None, 'tp'), P('tp', None))
    out_specs = (P('dp', None, None), P('dp', 'tp', None, None))
    return jax.shard_map(local_layer, mesh=mesh, in_specs=in_specs, out_specs=out_specs, check_vma=False)
```

```python
import jax
import jax.numpy as jnp
from jax import lax
from jax.experimental import pallas as pl
from jax.experimental.pallas import tpu as pltpu
from jax.sharding import PartitionSpec as P

NORM_EPS = 1e-5
GROUP_EPS = 1e-6
ROPE_BASE = 10000.0
CHUNK = 256
BLOCKS = 4
CHIPS = 4
F32 = jnp.float32
BF16 = jnp.bfloat16
MESH = pl.DeviceIdType.MESH


def normalize(x_f32, gain, bias):
    row_mean = jnp.mean(x_f32, axis=-1, keepdims=True)
    centered = x_f32 - row_mean
    variance = jnp.mean(centered * centered, axis=-1, keepdims=True)
    return centered * lax.rsqrt(variance + NORM_EPS) * gain + bias


def add_bf16(*terms):
    return sum(t.astype(F32) for t in terms).astype(BF16)


def layer_kernel(x_any, state_in, gain1, bias1, gain2, bias2, wq_any, wk_any, wv_any, wg_any, wo_any, up_any, down_any, base, table, decay, edge,
                 out_any, state_ref, up_all, down_all,
                 wq, wk, wv, wg, wo, wd, x_buf, part, met, own, rs, mid, hid, acc,
                 load_sem, x_sem, mid_sem, tile_sem, met_s, met_r, credit, rs_s, rs_r, z_s, z_r, f_s, f_r, g_s, g_r, p_s, p_r, ag_s, ag_r, agp_s, agp_r, put_sem):
    group, me = lax.axis_index('dp'), lax.axis_index('tp')
    chip, core = lax.div(me, 2), lax.rem(me, 2)
    partner = me + 1 - 2 * core
    across_x = lax.rem(group + 2, 4)
    across_y = group + 1 - 2 * lax.rem(group, 2)
    chunk = decay.shape[0]
    rows, share = own.shape[1], mid.shape[1]
    key_dim, half = wq.shape[1], wq.shape[1] // 2
    last = CHIPS - 1

    def remote(src, dst, s, r, **where):
        return pltpu.make_async_remote_copy(src_ref=src, dst_ref=dst, send_sem=s, recv_sem=r, device_id=where, device_id_type=MESH)

    weight_all, weight_own = (up_all, down_all), (up_any, down_any)
    quarter = tuple(w.shape[0] // 4 for w in weight_own)

    def piece(p, shard, q):
        return weight_all[p].at[shard, pl.ds(q * quarter[p], quarter[p])]

    def z_copy(side, hop, p):
        origin = chip - hop if side == 0 else chip + hop
        slot = piece(p, 2 * origin + core, group)
        src = weight_own[p].at[pl.ds(group * quarter[p], quarter[p])] if hop == 0 else slot
        return remote(src, slot, z_s.at[side, hop, p], z_r.at[origin, p], tp=me + 2 if side == 0 else me - 2)

    def first_copy(axis, origin, p, q=None):
        slot = piece(p, 2 * origin + core, group if q is None else q)
        return remote(slot, slot, f_s.at[axis, origin, p], f_r.at[axis, origin, p], dp=across_x if axis == 0 else across_y)

    def second_copy(origin, p, q=None):
        slot = piece(p, 2 * origin + core, (across_x if p == 0 else across_y) if q is None else q)
        return remote(slot, slot, g_s.at[origin, p], g_r.at[origin, p], dp=across_y if p == 0 else across_x)

    def partner_copy(origin, p, own_shard=False, incoming=False):
        slot = weight_all[p].at[2 * origin + (1 - core if incoming else core)]
        return remote(weight_own[p] if own_shard else slot, slot, p_s.at[origin, p], p_r.at[origin, p], tp=partner)

    def sides(d):
        return ((0, chip - d, chip >= d, chip < last), (1, chip + d, chip + d <= last, chip > 0))

    def spread_first(d):
        for side, origin, valid, onward in sides(d):
            @pl.when(valid)
            def _():
                for p in range(2):
                    remote(piece(p, 2 * origin + core, group), piece(p, 2 * origin + core, group), z_s.at[side, d - 1, p], z_r.at[origin, p], tp=partner).wait_recv()
                if d < last:
                    @pl.when(onward)
                    def _():
                        for p in range(2):
                            z_copy(side, d, p).start()
                for p in range(2):
                    for axis in range(2):
                        first_copy(axis, origin, p).start()

    def spread_second(d):
        for side, origin, valid, onward in sides(d):
            @pl.when(valid)
            def _():
                for p in range(2):
                    first_copy(0, origin, p, across_x).wait_recv()
                    first_copy(1, origin, p, across_y).wait_recv()
                for p in range(2):
                    second_copy(origin, p).start()

    def spread_third(d):
        for side, origin, valid, onward in sides(d):
            @pl.when(valid)
            def _():
                for p in range(2):
                    second_copy(origin, p, 3 - group).wait_recv()
                for p in range(2):
                    partner_copy(origin, p).start()

    def rs_copy(side, i, t, fresh):
        k = lax.rem(chip + (CHIPS - t if side == 0 else t), CHIPS)
        src = own.at[i, pl.ds(k * share, share)] if fresh else rs.at[side, i, t - 2]
        return remote(src, rs.at[side, i, t - 1], rs_s.at[side, i, t - 1], rs_r.at[side, i, t - 1], tp=me + 2 if side == 0 else me - 2)

    def rs_first(i):
        for side, end in ((0, 0), (1, last)):
            @pl.when(chip == end)
            def _():
                for t in range(1, CHIPS):
                    rs_copy(side, i, t, True).start()

    def rs_senders(side, t):
        return (chip >= 1) & (chip <= t - 1) & (chip < last) if side == 0 else (chip < last) & (chip >= CHIPS - t) & (chip >= 1)

    def rs_step(i, t):
        for side in range(2):
            @pl.when(rs_senders(side, t))
            def _():
                rs_copy(side, i, t - 1, False if t > 2 else True).wait_recv()
                k = lax.rem(chip + (CHIPS - t if side == 0 else t), CHIPS)
                rs[side, i, t - 2] = add_bf16(rs[side, i, t - 2], own[i, pl.ds(pl.multiple_of(k * share, share), share)])
                rs_copy(side, i, t, False).start()

    def rs_final(i):
        mine = lambda: own[i, pl.ds(pl.multiple_of(chip * share, share), share)]

        @pl.when(chip >= 1)
        def _():
            rs_copy(0, i, last, True).wait_recv()

        @pl.when(chip < last)
        def _():
            rs_copy(1, i, last, True).wait_recv()

        @pl.when(chip == 0)
        def _():
            mid[i] = add_bf16(mid[i], add_bf16(mine(), rs[1, i, last - 1]))

        @pl.when(chip == last)
        def _():
            mid[i] = add_bf16(mid[i], add_bf16(mine(), rs[0, i, last - 1]))

        @pl.when((chip >= 1) & (chip < last))
        def _():
            mid[i] = add_bf16(mid[i], add_bf16(mine(), rs[0, i, last - 1], rs[1, i, last - 1]))

    def ag_copy(g, side, hop):
        origin = chip - hop if side == 0 else chip + hop
        slot = out_any.at[core, pl.ds(2 * g, 2), origin]
        src = mid.at[pl.ds(2 * g, 2)] if hop == 0 else slot
        return remote(src, slot, ag_s.at[g, side, hop], ag_r.at[g, origin], tp=me + 2 if side == 0 else me - 2)

    def agp_copy(g, origin, fresh=False, incoming=False):
        slot = out_any.at[1 - core if incoming else core, pl.ds(2 * g, 2), origin]
        return remote(mid.at[pl.ds(2 * g, 2)] if fresh else slot, slot, agp_s.at[g, origin], agp_r.at[g, origin], tp=partner)

    def put_copy(g):
        return pltpu.make_async_copy(mid.at[pl.ds(2 * g, 2)], out_any.at[core, pl.ds(2 * g, 2), chip], put_sem.at[g])

    def ag_first(g):
        put_copy(g).start()

        @pl.when(chip < last)
        def _():
            ag_copy(g, 0, 0).start()

        @pl.when(chip > 0)
        def _():
            ag_copy(g, 1, 0).start()

        agp_copy(g, chip, fresh=True).start()

    def ag_step(g, d):
        for side, origin, valid, onward in sides(d):
            @pl.when(valid)
            def _():
                slot = out_any.at[core, pl.ds(2 * g, 2), origin]
                remote(slot, slot, ag_s.at[g, side, d - 1], ag_r.at[g, origin], tp=partner).wait_recv()
                if d < last:
                    @pl.when(onward)
                    def _():
                        ag_copy(g, side, d).start()
                agp_copy(g, origin).start()

    def x_copy(n):
        seq = core + (1 - 2 * core) * (1 - lax.rem(n, 2))
        return pltpu.make_async_copy(x_any.at[seq, lax.div(n, 2)], x_buf.at[lax.rem(n, 2)], x_sem.at[lax.rem(n, 2)])

    def met_copy(i):
        return remote(part, met.at[lax.rem(i, 2)], met_s, met_r.at[lax.rem(i, 2)], tp=partner)

    barrier = pltpu.get_barrier_semaphore()
    for where in ({'tp': partner}, {'dp': across_x}, {'dp': across_y}):
        pl.semaphore_signal(barrier, inc=1, device_id=where, device_id_type=MESH)

    @pl.when(chip < last)
    def _():
        pl.semaphore_signal(barrier, inc=1, device_id={'tp': me + 2}, device_id_type=MESH)

    @pl.when(chip > 0)
    def _():
        pl.semaphore_signal(barrier, inc=1, device_id={'tp': me - 2}, device_id_type=MESH)

    loads = [pltpu.make_async_copy(a, b, load_sem.at[k]) for k, (a, b) in enumerate(((wq_any, wq), (wk_any, wk), (wv_any, wv), (wg_any, wg), (wo_any, wo)))]
    x_copy(0).start()
    for load in loads:
        load.start()
    mid_load = pltpu.make_async_copy(x_any.at[core, :, chip], mid, mid_sem)
    mid_load.start()
    pl.semaphore_wait(barrier, 3 + (chip < last).astype(jnp.int32) + (chip > 0).astype(jnp.int32))

    for p in range(2):
        @pl.when(chip < last)
        def _():
            z_copy(0, 0, p).start()

        @pl.when(chip > 0)
        def _():
            z_copy(1, 0, p).start()

        partner_copy(chip, p, own_shard=True).start()

    state_ref[...] = state_in[...]
    for load in loads:
        load.wait()

    def attend(n, carry):
        i, k = lax.div(n, 2), lax.rem(n, 2)
        seq = core + (1 - 2 * core) * (1 - k)
        x_copy(n).wait()

        @pl.when(n < 2 * BLOCKS - 1)
        def _():
            x_copy(n + 1).start()

        h = normalize(x_buf[k].reshape(rows, part.shape[1]).astype(F32), gain1[...], bias1[...]).astype(BF16)
        q_raw = jnp.dot(h, wq[...], preferred_element_type=F32)
        k_raw = jnp.dot(h, wk[...], preferred_element_type=F32)
        v_all = jnp.dot(h, wv[...], preferred_element_type=F32).astype(BF16)
        g_all = jnp.dot(h, wg[...], preferred_element_type=F32)
        cos_lo, sin_lo = table[0], table[1]
        mixed = []
        subs = rows // chunk
        for sub in range(subs):
            span = slice(sub * chunk, (sub + 1) * chunk)
            cos_hi, sin_hi = base[seq, i * subs + sub, 0:1, :], base[seq, i * subs + sub, 1:2, :]
            cos_t = cos_hi * cos_lo - sin_hi * sin_lo
            sin_t = sin_hi * cos_lo + cos_hi * sin_lo

            def rotate(raw):
                first, second = raw[span, :half], raw[span, half:]
                return jnp.concatenate([first * cos_t - second * sin_t, second * cos_t + first * sin_t], axis=-1)

            queries = rotate(q_raw).astype(BF16)
            keys = (rotate(k_raw) * key_dim ** -0.5).astype(BF16)
            values = v_all[span]
            state = state_ref[seq, 0]
            scores = lax.dot_general(queries, keys, (((1,), (1,)), ((), ())), preferred_element_type=F32) * decay[...]
            retained = jnp.dot(scores.astype(BF16), values, preferred_element_type=F32)
            retained += jnp.dot(queries, state.astype(BF16), preferred_element_type=F32) * edge[:, 0:1]
            keys_decayed = (keys.astype(F32) * edge[:, 1:2]).astype(BF16)
            grown = lax.dot_general(keys_decayed, values, (((0,), (0,)), ((), ())), preferred_element_type=F32)
            state_ref[seq, 0] = state * edge[0:1, 2:3] + grown
            row_mean = jnp.mean(retained, axis=-1, keepdims=True)
            centered = retained - row_mean
            variance = jnp.mean(centered * centered, axis=-1, keepdims=True)
            normed = centered * lax.rsqrt(variance + GROUP_EPS)
            mixed.append((jax.nn.silu(g_all[span]) * normed).astype(BF16))
        u = jnp.dot(jnp.concatenate(mixed, axis=0), wo[...], preferred_element_type=F32).astype(BF16)

        @pl.when(k == 1)
        def _():
            met_copy(i).wait_send()

        part[...] = u

        @pl.when(k == 0)
        def _():
            @pl.when(i >= 2)
            def _():
                pl.semaphore_wait(credit, 1)

            met_copy(i).start()

        @pl.when(k == 1)
        def _():
            met_copy(i).wait_recv()
            own[i] = add_bf16(part[...], met[lax.rem(i, 2)])

            @pl.when(i < BLOCKS - 2)
            def _():
                pl.semaphore_signal(credit, inc=1, device_id={'tp': partner}, device_id_type=MESH)

            rs_first(i)

            @pl.when(i >= 1)
            def _():
                rs_step(i - 1, 2)

            @pl.when(i >= 2)
            def _():
                rs_step(i - 2, 3)

        @pl.when(n == 2)
        def _():
            spread_first(1)

        @pl.when(n == 4)
        def _():
            spread_first(2)
            spread_second(1)

        @pl.when(n == 6)
        def _():
            spread_second(2)
            spread_third(1)

        @pl.when(n == 7)
        def _():
            spread_first(3)

        return carry

    lax.fori_loop(0, 2 * BLOCKS, attend, 0)

    mid_load.wait()

    def shard_of(e, other):
        origin = chip if e == 0 else chip + 1 - 2 * lax.rem(chip, 2) if e == 1 else 2 - lax.div(chip, 2) if e == 2 else 3 - 3 * lax.div(chip, 2)
        return origin, 2 * origin + (1 - core if other else core)

    slots = ((wv, wo), (wg, wd))

    def tile_copies(step):
        e, other = step // 2, step % 2
        shard = shard_of(e, other)[1]
        sources = (up_any, down_any) if step == 0 else (up_all.at[shard], down_all.at[shard])
        return [pltpu.make_async_copy(sources[p], slots[step % 2][p], tile_sem.at[step % 2, p]) for p in range(2)]

    def arrive(step):
        e, other = step // 2, step % 2
        if other:
            for p in range(2):
                partner_copy(shard_of(e, 0)[0], p, incoming=True).wait_recv()
        elif e > 0:
            spread_third(e) if e > 1 else None

    def feed_forward(g):
        width = mid.shape[2]
        for copy in tile_copies(0):
            copy.start()
        x_mid = mid[pl.ds(2 * g, 2)].reshape(2 * share, width).astype(F32)
        hid[...] = normalize(x_mid, gain2[...], bias2[...]).astype(BF16)
        for step in range(2 * CHIPS):
            if step + 1 < 2 * CHIPS:
                if g == 0:
                    arrive(step + 1)
                for copy in tile_copies(step + 1):
                    copy.start()
            for copy in tile_copies(step):
                copy.wait()
            up, down = slots[step % 2]
            pre = jnp.dot(hid[...], up[...], preferred_element_type=F32)
            act = (0.5 * pre * (1.0 + lax.erf(pre * 0.5 ** 0.5))).astype(BF16)
            grown = jnp.dot(act, down[...], preferred_element_type=F32)
            acc[...] = grown if step == 0 else acc[...] + grown
        f = acc[...].astype(BF16).astype(F32)
        x_mid = mid[pl.ds(2 * g, 2)].reshape(2 * share, width).astype(F32)
        mid[pl.ds(2 * g, 2)] = (x_mid + f).astype(BF16).reshape(2, share, width)

    rs_final(0)
    rs_final(1)
    spread_second(3)
    feed_forward(0)
    ag_first(0)
    rs_step(2, 3)
    rs_step(3, 2)
    rs_step(3, 3)
    rs_final(2)
    rs_final(3)
    ag_step(0, 1)
    feed_forward(1)
    ag_first(1)
    for d in range(1, CHIPS):
        if d > 1:
            ag_step(0, d)
        ag_step(1, d) if d < 2 else None
    ag_step(1, 2)
    ag_step(1, 3)

    for g in range(2):
        put_copy(g).wait()
        for origin in range(CHIPS):
            agp_copy(g, origin).wait_send()
            agp_copy(g, origin, incoming=True).wait_recv()
        for hop in range(last):
            @pl.when((chip >= hop) & (chip < last))
            def _():
                ag_copy(g, 0, hop).wait_send()

            @pl.when((chip + hop <= last) & (chip > 0))
            def _():
                ag_copy(g, 1, hop).wait_send()
    for p in range(2):
        partner_copy(chip, p, own_shard=True).wait_send()
        for hop in range(last):
            @pl.when((chip >= hop) & (chip < last))
            def _():
                z_copy(0, hop, p).wait_send()

            @pl.when((chip + hop <= last) & (chip > 0))
            def _():
                z_copy(1, hop, p).wait_send()
        for d in range(1, CHIPS):
            for side, origin, valid, onward in sides(d):
                @pl.when(valid)
                def _():
                    partner_copy(origin, p).wait_send()
                    second_copy(origin, p).wait_send()
                    for axis in range(2):
                        first_copy(axis, origin, p).wait_send()

    def settle(i, carry):
        for side, end in ((0, 0), (1, last)):
            for t in range(1, CHIPS):
                @pl.when((chip == end) | (rs_senders(side, t) if t > 1 else chip < 0))
                def _():
                    rs_copy(side, i, t, True).wait_send()
        return carry

    lax.fori_loop(0, BLOCKS, settle, 0)


def solution(mesh):
    members = mesh.shape['tp']

    def local_layer(x_in, start_pos, kv_state, ln1_gain, ln1_bias, w_q, w_k, w_v, w_g, w_o, ln2_gain, ln2_bias, w_up, w_down):
        seqs, chunk_len, d_model = x_in.shape
        key_dim = kv_state.shape[2]
        half = key_dim // 2
        rows = chunk_len // BLOCKS
        share = rows // CHIPS
        chunk = min(CHUNK, rows)
        me = lax.axis_index('tp')
        log_gamma = jnp.log1p(-jnp.exp2(-5.0 - me.astype(F32)))
        ids = jnp.arange(chunk)
        gap = ids[:, None] - ids[None, :]
        decay = jnp.where(gap >= 0, jnp.exp(jnp.maximum(gap, 0).astype(F32) * log_gamma), 0.0)
        lane = jnp.arange(128)[None, :]
        power = jnp.where(lane == 0, ids[:, None] + 1, jnp.where(lane == 1, chunk - 1 - ids[:, None], chunk))
        edge = jnp.exp(power.astype(F32) * log_gamma)
        inv_freq = jnp.power(ROPE_BASE, -jnp.arange(half).astype(F32) / half)
        low = ids.astype(F32)[:, None] * inv_freq[None, :]
        table = jnp.stack([jnp.cos(low), jnp.sin(low)])
        high = (start_pos[:, None] + jnp.arange(chunk_len // chunk)[None, :] * chunk).astype(F32)[:, :, None] * inv_freq
        base = jnp.stack([jnp.cos(high), jnp.sin(high)], axis=2)

        anywhere = pl.BlockSpec(memory_space=pl.ANY)
        vmem = pl.BlockSpec(memory_space=pltpu.VMEM)
        dma = lambda *shape: pltpu.SemaphoreType.DMA(shape)
        out, state, _, _ = pl.pallas_call(
            layer_kernel,
            in_specs=[anywhere, vmem, vmem, vmem, vmem, vmem] + [anywhere] * 7 + [vmem] * 4,
            out_specs=[anywhere, vmem, anywhere, anywhere],
            out_shape=[
                jax.ShapeDtypeStruct((seqs, BLOCKS, CHIPS, share, d_model), BF16),
                jax.ShapeDtypeStruct(kv_state.shape, F32),
                jax.ShapeDtypeStruct((members,) + w_up.shape, BF16),
                jax.ShapeDtypeStruct((members,) + w_down.shape, BF16),
            ],
            scratch_shapes=[
                pltpu.VMEM(w_q.shape, BF16), pltpu.VMEM(w_k.shape, BF16), pltpu.VMEM(w_v.shape, BF16), pltpu.VMEM(w_g.shape, BF16),
                pltpu.VMEM(w_o.shape, BF16), pltpu.VMEM(w_down.shape, BF16),
                pltpu.VMEM((2, CHIPS, share, d_model), BF16), pltpu.VMEM((rows, d_model), BF16), pltpu.VMEM((2, rows, d_model), BF16),
                pltpu.VMEM((BLOCKS, rows, d_model), BF16), pltpu.VMEM((2, BLOCKS, CHIPS - 1, share, d_model), BF16),
                pltpu.VMEM((BLOCKS, share, d_model), BF16), pltpu.VMEM((2 * share, d_model), BF16), pltpu.VMEM((2 * share, d_model), F32),
                dma(5), dma(2), pltpu.SemaphoreType.DMA, dma(2, 2), pltpu.SemaphoreType.DMA, dma(2), pltpu.SemaphoreType.REGULAR,
                dma(2, BLOCKS, 3), dma(2, BLOCKS, 3), dma(2, 3, 2), dma(4, 2), dma(2, 4, 2), dma(2, 4, 2), dma(4, 2), dma(4, 2), dma(4, 2), dma(4, 2),
                dma(2, 2, 3), dma(2, 4), dma(2, 4), dma(2, 4), dma(2),
            ],
            compiler_params=pltpu.CompilerParams(collective_id=0, has_side_effects=True, vmem_limit_bytes=67043328),
            name="layer",
        )(x_in.reshape(seqs, BLOCKS, CHIPS, share, d_model), kv_state, *(a[None, :] for a in (ln1_gain, ln1_bias, ln2_gain, ln2_bias)), w_q, w_k, w_v, w_g, w_o, w_up, w_down, base, table, decay, edge)
        return out.reshape(seqs, chunk_len, d_model), state

    in_specs = (P('dp', None, None), P('dp'), P('dp', 'tp', None, None), P(), P(), P(None, 'tp'), P(None, 'tp'), P(None, 'tp'), P(None, 'tp'), P('tp', None), P(), P(), P(None, 'tp'), P('tp', None))
    out_specs = (P('dp', None, None), P('dp', 'tp', None, None))
    return jax.shard_map(local_layer, mesh=mesh, in_specs=in_specs, out_specs=out_specs, check_vma=False)
```

```python
import jax
import jax.numpy as jnp
from jax import lax
from jax.experimental import pallas as pl
from jax.experimental.pallas import tpu as pltpu
from jax.sharding import PartitionSpec as P

NORM_EPS = 1e-5
GROUP_EPS = 1e-6
ROPE_BASE = 10000.0
CHUNK = 256
BLOCKS = 4
CHIPS = 4
F32 = jnp.float32
BF16 = jnp.bfloat16
MESH = pl.DeviceIdType.MESH
GROUPS = ((0, 1), (2,), (3,))
LOOP = {
    0: (
        ('s1', 'm', 'f1', 0), ('s1', 'm', 'n1', 1), ('s1', 'm', 'f1', 1),
    ),
    1: (
        ('s1', 'm', 'n1', 0),
    ),
    2: (
        ('s1', 'e', 1, 0),
    ),
    3: (
        ('s1', 'e', 1, 1), ('s1', 'e', 2, 0), ('s2', 'e', 1, 1), ('s1', 'm', 'f2', 0), ('rs', 'm', 0, 2, 'n'), ('s2', 'e', 1, 0),
        ('rs', 'm', 0, 3, 'n'), ('s1', 'e', 3, 0), ('s1', 'm', 'f2', 1), ('s2', 'm', 'f1', 1), ('s3', 'e', 1, 0), ('s3', 'e', 1, 1),
    ),
    5: (
        ('rs', 'm', 1, 2, 'n'),
    ),
    6: (
        ('s2', 'm', 'n1', 1), ('s2', 'm', 'n1', 0), ('fin', 'm', 0), ('s1', 'e', 3, 1),
    ),
}
TAIL = (
    ('rs', 'm', 1, 3, 'n'), ('s1', 'e', 2, 1), ('s2', 'm', 'f1', 0), ('rs', 'm', 1, 3, 'f'), ('rs', 'm', 0, 3, 'f'), ('fin', 'e', 1),
    ('s3', 'm', 'f1', 1), ('s3', 'm', 'n1', 0), ('s2', 'm', 'f2', 1), ('s2', 'e', 2, 0), ('s2', 'm', 'f2', 0), ('fin', 'm', 1),
    ('rs', 'm', 2, 2, 'n'), ('fin', 'e', 0), ('s3', 'm', 'n1', 1), ('F', 0, 0), ('s2', 'e', 3, 1), ('s3', 'e', 2, 0), ('s3', 'm', 'f1', 0),
    ('F', 0, 1), ('s2', 'e', 3, 0), ('s2', 'e', 2, 1), ('s3', 'e', 3, 0), ('s3', 'e', 2, 1), ('fin', 'e', 2), ('F', 0, 2), ('F', 0, 3),
    ('rs', 'm', 2, 3, 'n'), ('s3', 'm', 'f2', 0), ('s3', 'm', 'f2', 1), ('rs', 'm', 2, 3, 'f'), ('s3', 'e', 3, 1), ('F', 0, 4),
    ('ag', 'e', 1, 0), ('F', 0, 5), ('F', 0, 6), ('F', 0, 7), ('agf', 0), ('fin', 'm', 2), ('F', 1, 0), ('F', 1, 1), ('F', 1, 2),
    ('rs', 'm', 3, 2, 'n'), ('F', 1, 3), ('F', 1, 4), ('rs', 'm', 3, 3, 'n'), ('F', 1, 5), ('ag', 'm', 'f1', 0), ('ag', 'e', 1, 2),
    ('F', 1, 6), ('ag', 'm', 'f1', 1), ('F', 1, 7), ('rs', 'm', 3, 3, 'f'), ('ag', 'm', 'n1', 0), ('agf', 1), ('fin', 'e', 3),
    ('fin', 'm', 3), ('ag', 'e', 1, 1), ('F', 2, 0), ('F', 2, 1), ('F', 2, 2), ('F', 2, 3), ('F', 2, 4), ('F', 2, 5), ('F', 2, 6),
    ('ag', 'e', 2, 1), ('F', 2, 7), ('ag', 'm', 'f2', 0), ('agf', 2), ('ag', 'm', 'n1', 1), ('ag', 'e', 3, 0), ('ag', 'e', 2, 3),
    ('ag', 'e', 3, 1), ('ag', 'e', 3, 2), ('ag', 'm', 'n1', 2), ('ag', 'm', 'f1', 3), ('ag', 'm', 'f1', 2), ('ag', 'e', 2, 2),
    ('ag', 'm', 'n1', 3), ('ag', 'm', 'f2', 2), ('ag', 'e', 1, 3), ('ag', 'e', 2, 0), ('ag', 'm', 'f2', 1), ('ag', 'm', 'f2', 3),
    ('ag', 'e', 3, 3),
)


def normalize(x_f32, gain, bias):
    row_mean = jnp.mean(x_f32, axis=-1, keepdims=True)
    centered = x_f32 - row_mean
    variance = jnp.mean(centered * centered, axis=-1, keepdims=True)
    return centered * lax.rsqrt(variance + NORM_EPS) * gain + bias


def add_bf16(*terms):
    return sum(t.astype(F32) for t in terms).astype(BF16)


def layer_kernel(x_any, state_in, gain1, bias1, gain2, bias2, wq_any, wk_any, wv_any, wg_any, wo_any, up_any, down_any, base, table, decay, edge,
                 out_any, state_ref, up_all, down_all,
                 wq, wk, wv, wg, wo, wd, x_buf, part, met, own, rs, mid, hid, acc,
                 load_sem, x_sem, mid_sem, tile_sem, met_s, met_r, credit, rs_s, rs_r, z_s, z_r, f_s, f_r, g_s, g_r, p_s, p_r, ag_s, ag_r, agp_s, agp_r, put_sem):
    group, me = lax.axis_index('dp'), lax.axis_index('tp')
    chip, core = lax.div(me, 2), lax.rem(me, 2)
    partner = me + 1 - 2 * core
    across_x = lax.rem(group + 2, 4)
    across_y = group + 1 - 2 * lax.rem(group, 2)
    chunk = decay.shape[0]
    rows, share = own.shape[1], mid.shape[1]
    key_dim, half = wq.shape[1], wq.shape[1] // 2
    last = CHIPS - 1
    far = 1 - 2 * lax.div(chip, 2)
    is_end = (chip == 0) | (chip == last)
    is_middle = (chip > 0) & (chip < last)

    def remote(src, dst, s, r, **where):
        return pltpu.make_async_remote_copy(src_ref=src, dst_ref=dst, send_sem=s, recv_sem=r, device_id=where, device_id_type=MESH)

    def side_of(flow):
        return lax.div(1 - flow, 2)

    weight_all, weight_own = (up_all, down_all), (up_any, down_any)
    quarter = tuple(w.shape[0] // 4 for w in weight_own)

    def origin_of(which):
        return {'n1': chip - far, 'f1': chip + far, 'f2': chip + 2 * far}[which] if isinstance(which, str) else chip + which * far

    def piece(p, shard, q):
        return weight_all[p].at[shard, pl.ds(q * quarter[p], quarter[p])]

    def z_copy(flow, origin, p, own_piece=False):
        slot = piece(p, 2 * origin + core, group)
        src = weight_own[p].at[pl.ds(group * quarter[p], quarter[p])] if own_piece else slot
        return remote(src, slot, z_s.at[side_of(flow), origin, p], z_r.at[origin, p], tp=me + 2 * flow)

    def first_copy(axis, origin, p, q=None):
        slot = piece(p, 2 * origin + core, group if q is None else q)
        return remote(slot, slot, f_s.at[axis, origin, p], f_r.at[axis, origin, p], dp=across_x if axis == 0 else across_y)

    def second_copy(origin, p, q=None):
        slot = piece(p, 2 * origin + core, (across_x if p == 0 else across_y) if q is None else q)
        return remote(slot, slot, g_s.at[origin, p], g_r.at[origin, p], dp=across_y if p == 0 else across_x)

    def partner_copy(origin, p, own_shard=False, incoming=False):
        slot = weight_all[p].at[2 * origin + (1 - core if incoming else core)]
        return remote(weight_own[p] if own_shard else slot, slot, p_s.at[origin, p], p_r.at[origin, p], tp=partner)

    def spread_first(which, p):
        origin = origin_of(which)
        z_copy(far, origin, p).wait_recv()
        if isinstance(which, str):
            z_copy(far if which == 'n1' else -far, origin, p).start()
        for axis in range(2):
            first_copy(axis, origin, p).start()

    def spread_second(which, p):
        origin = origin_of(which)
        first_copy(p, origin, p, across_x if p == 0 else across_y).wait_recv()
        second_copy(origin, p).start()

    def spread_third(which, p):
        origin = origin_of(which)
        first_copy(1 - p, origin, p, across_y if p == 0 else across_x).wait_recv()
        second_copy(origin, p, 3 - group).wait_recv()
        partner_copy(origin, p).start()

    def rs_shard(flow, t):
        return lax.rem(chip - flow * t + CHIPS, CHIPS)

    def rs_copy(flow, i, t, fresh=False):
        side = side_of(flow)
        src = own.at[i, pl.ds(rs_shard(flow, t) * share, share)] if fresh else rs.at[side, i, t - 2]
        return remote(src, rs.at[side, i, t - 1], rs_s.at[side, i, t - 1], rs_r.at[side, i, t - 1], tp=me + 2 * flow)

    def rs_first(i):
        @pl.when(is_end)
        def _():
            for t in range(1, CHIPS):
                rs_copy(far, i, t, fresh=True).start()

    def mine(i, k):
        return own[i, pl.ds(pl.multiple_of(k * share, share), share)]

    def rs_step(i, t, which):
        flow = far if which == 'n' else -far
        side = side_of(flow)
        rs_copy(flow, i, t - 1, fresh=True).wait_recv()
        rs[side, i, t - 2] = add_bf16(rs[side, i, t - 2], mine(i, rs_shard(flow, t)))
        rs_copy(flow, i, t).start()

    def rs_final(kind, i):
        rs_copy(-far, i, last, fresh=True).wait_recv()
        terms = [mine(i, chip), rs[side_of(-far), i, last - 1]]
        if kind == 'm':
            rs_copy(far, i, last, fresh=True).wait_recv()
            terms.append(rs[side_of(far), i, last - 1])
        mid[i] = add_bf16(mid[i], add_bf16(*terms))

    def ag_copy(b, flow, origin, fresh=False):
        slot = out_any.at[core, b, origin]
        return remote(mid.at[b] if fresh else slot, slot, ag_s.at[b, side_of(flow), origin], ag_r.at[b, origin], tp=me + 2 * flow)

    def agp_copy(b, origin, fresh=False, incoming=False):
        slot = out_any.at[1 - core if incoming else core, b, origin]
        return remote(mid.at[b] if fresh else slot, slot, agp_s.at[b, origin], agp_r.at[b, origin], tp=partner)

    def put_copy(b):
        return pltpu.make_async_copy(mid.at[b], out_any.at[core, b, chip], put_sem.at[b])

    def ag_first(g):
        for b in GROUPS[g]:
            ag_copy(b, far, chip, fresh=True).start()

            @pl.when(is_middle)
            def _():
                ag_copy(b, -far, chip, fresh=True).start()

            agp_copy(b, chip, fresh=True).start()
            put_copy(b).start()

    def ag_step(which, b):
        origin = origin_of(which)
        ag_copy(b, far, origin).wait_recv()
        if isinstance(which, str):
            ag_copy(b, far if which == 'n1' else -far, origin).start()
        agp_copy(b, origin).start()

    def serve(item):
        kind, where, args = item[0], item[1], item[2:]

        @pl.when(is_end if where == 'e' else is_middle)
        def _():
            if kind == 's1':
                spread_first(*args)
            elif kind == 's2':
                spread_second(*args)
            elif kind == 's3':
                spread_third(*args)
            elif kind == 'rs':
                rs_step(*args)
            elif kind == 'fin':
                rs_final(where, *args)
            else:
                ag_step(*args)

    def x_copy(n):
        seq = core + (1 - 2 * core) * (1 - lax.rem(n, 2))
        return pltpu.make_async_copy(x_any.at[seq, lax.div(n, 2)], x_buf.at[lax.rem(n, 2)], x_sem.at[lax.rem(n, 2)])

    def met_copy(i):
        return remote(part, met.at[lax.rem(i, 2)], met_s, met_r.at[lax.rem(i, 2)], tp=partner)

    barrier = pltpu.get_barrier_semaphore()
    for where in ({'tp': partner}, {'dp': across_x}, {'dp': across_y}):
        pl.semaphore_signal(barrier, inc=1, device_id=where, device_id_type=MESH)

    @pl.when(chip < last)
    def _():
        pl.semaphore_signal(barrier, inc=1, device_id={'tp': me + 2}, device_id_type=MESH)

    @pl.when(chip > 0)
    def _():
        pl.semaphore_signal(barrier, inc=1, device_id={'tp': me - 2}, device_id_type=MESH)

    loads = [pltpu.make_async_copy(a, b, load_sem.at[k]) for k, (a, b) in enumerate(((wq_any, wq), (wk_any, wk), (wv_any, wv), (wg_any, wg), (wo_any, wo)))]
    x_copy(0).start()
    for load in loads:
        load.start()
    mid_load = pltpu.make_async_copy(x_any.at[core, :, chip], mid, mid_sem)
    mid_load.start()
    pl.semaphore_wait(barrier, 4 + is_middle.astype(jnp.int32))

    for p in range(2):
        z_copy(far, chip, p, own_piece=True).start()

        @pl.when(is_middle)
        def _():
            z_copy(-far, chip, p, own_piece=True).start()

        partner_copy(chip, p, own_shard=True).start()

    state_ref[...] = state_in[...]
    for load in loads:
        load.wait()
    mid_load.wait()

    def attend(n, carry):
        i, k = lax.div(n, 2), lax.rem(n, 2)
        seq = core + (1 - 2 * core) * (1 - k)
        x_copy(n).wait()

        @pl.when(n < 2 * BLOCKS - 1)
        def _():
            x_copy(n + 1).start()

        h = normalize(x_buf[k].reshape(rows, part.shape[1]).astype(F32), gain1[...], bias1[...]).astype(BF16)
        q_raw = jnp.dot(h, wq[...], preferred_element_type=F32)
        k_raw = jnp.dot(h, wk[...], preferred_element_type=F32)
        v_all = jnp.dot(h, wv[...], preferred_element_type=F32).astype(BF16)
        g_all = jnp.dot(h, wg[...], preferred_element_type=F32)
        cos_lo, sin_lo = table[0], table[1]
        mixed = []
        subs = rows // chunk
        for sub in range(subs):
            span = slice(sub * chunk, (sub + 1) * chunk)
            cos_hi, sin_hi = base[seq, i * subs + sub, 0:1, :], base[seq, i * subs + sub, 1:2, :]
            cos_t = cos_hi * cos_lo - sin_hi * sin_lo
            sin_t = sin_hi * cos_lo + cos_hi * sin_lo

            def rotate(raw):
                first, second = raw[span, :half], raw[span, half:]
                return jnp.concatenate([first * cos_t - second * sin_t, second * cos_t + first * sin_t], axis=-1)

            queries = rotate(q_raw).astype(BF16)
            keys = (rotate(k_raw) * key_dim ** -0.5).astype(BF16)
            values = v_all[span]
            state = state_ref[seq, 0]
            scores = lax.dot_general(queries, keys, (((1,), (1,)), ((), ())), preferred_element_type=F32) * decay[...]
            retained = jnp.dot(scores.astype(BF16), values, preferred_element_type=F32)
            retained += jnp.dot(queries, state.astype(BF16), preferred_element_type=F32) * edge[:, 0:1]
            keys_decayed = (keys.astype(F32) * edge[:, 1:2]).astype(BF16)
            grown = lax.dot_general(keys_decayed, values, (((0,), (0,)), ((), ())), preferred_element_type=F32)
            state_ref[seq, 0] = state * edge[0:1, 2:3] + grown
            row_mean = jnp.mean(retained, axis=-1, keepdims=True)
            centered = retained - row_mean
            variance = jnp.mean(centered * centered, axis=-1, keepdims=True)
            normed = centered * lax.rsqrt(variance + GROUP_EPS)
            mixed.append((jax.nn.silu(g_all[span]) * normed).astype(BF16))
        u = jnp.dot(jnp.concatenate(mixed, axis=0), wo[...], preferred_element_type=F32).astype(BF16)

        @pl.when(k == 1)
        def _():
            met_copy(i).wait_send()

        part[...] = u

        @pl.when(k == 0)
        def _():
            @pl.when(i >= 2)
            def _():
                pl.semaphore_wait(credit, 1)

            met_copy(i).start()

        @pl.when(k == 1)
        def _():
            met_copy(i).wait_recv()
            own[i] = add_bf16(part[...], met[lax.rem(i, 2)])

            @pl.when(i < BLOCKS - 2)
            def _():
                pl.semaphore_signal(credit, inc=1, device_id={'tp': partner}, device_id_type=MESH)

            rs_first(i)

        for turn, items in LOOP.items():
            @pl.when(n == turn)
            def _():
                for item in items:
                    serve(item)

        return carry

    lax.fori_loop(0, 2 * BLOCKS, attend, 0)

    def origin_at(e):
        return (chip, chip + 1 - 2 * lax.rem(chip, 2), 2 - lax.div(chip, 2), 3 - 3 * lax.div(chip, 2))[e]

    slots = ((wv, wo), (wg, wd))

    def tile_copies(step):
        shard = 2 * origin_at(step // 2) + (1 - core if step % 2 else core)
        sources = (up_any, down_any) if step == 0 else (up_all.at[shard], down_all.at[shard])
        return [pltpu.make_async_copy(sources[p], slots[step % 2][p], tile_sem.at[step % 2, p]) for p in range(2)]

    def ffn_tile(height, step):
        for copy in tile_copies(step):
            copy.wait()
        up, down = slots[step % 2]
        pre = jnp.dot(hid[:height], up[...], preferred_element_type=F32)
        act = (0.5 * pre * (1.0 + lax.erf(pre * 0.5 ** 0.5))).astype(BF16)
        grown = jnp.dot(act, down[...], preferred_element_type=F32)
        acc[:height] = grown if step == 0 else acc[:height] + grown

    def ffn_step(g, step):
        first, count = GROUPS[g][0], len(GROUPS[g])
        height, width = count * share, mid.shape[2]
        x_mid = lambda: mid[first:first + count].reshape(height, width).astype(F32)
        if g == 0 and step % 2:
            for p in range(2):
                partner_copy(origin_at(step // 2), p, incoming=True).wait_recv()
        for copy in tile_copies(step):
            copy.start()
        if step == 0:
            hid[:height] = normalize(x_mid(), gain2[...], bias2[...]).astype(BF16)
        else:
            ffn_tile(height, step - 1)
        if step == 2 * CHIPS - 1:
            ffn_tile(height, step)
            f = acc[:height].astype(BF16).astype(F32)
            mid[first:first + count] = (x_mid() + f).astype(BF16).reshape(count, share, width)

    for item in TAIL:
        if item[0] == 'F':
            ffn_step(*item[1:])
        elif item[0] == 'agf':
            ag_first(*item[1:])
        else:
            serve(item)

    for b in range(BLOCKS):
        put_copy(b).wait()
        ag_copy(b, far, chip).wait_send()
        for origin in range(CHIPS):
            agp_copy(b, origin).wait_send()
            agp_copy(b, origin, incoming=True).wait_recv()
    for p in range(2):
        z_copy(far, chip, p).wait_send()
        partner_copy(chip, p, own_shard=True).wait_send()

    def settle_weights(which):
        for p in range(2):
            origin = origin_of(which)
            partner_copy(origin, p).wait_send()
            second_copy(origin, p).wait_send()
            for axis in range(2):
                first_copy(axis, origin, p).wait_send()
            if isinstance(which, str):
                z_copy(far if which == 'n1' else -far, origin, p).wait_send()

    @pl.when(is_end)
    def _():
        for which in (1, 2, 3):
            settle_weights(which)
        for i in range(BLOCKS):
            for t in range(1, CHIPS):
                rs_copy(far, i, t, fresh=True).wait_send()

    @pl.when(is_middle)
    def _():
        for which in ('n1', 'f1', 'f2'):
            settle_weights(which)
        for p in range(2):
            z_copy(-far, chip, p).wait_send()
        for i in range(BLOCKS):
            for flow, t in ((far, 2), (far, 3), (-far, 3)):
                rs_copy(flow, i, t).wait_send()
            ag_copy(i, -far, chip).wait_send()
            for which in ('n1', 'f1', 'f2'):
                ag_copy(i, far if which == 'n1' else -far, origin_of(which)).wait_send()


def solution(mesh):
    members = mesh.shape['tp']

    def local_layer(x_in, start_pos, kv_state, ln1_gain, ln1_bias, w_q, w_k, w_v, w_g, w_o, ln2_gain, ln2_bias, w_up, w_down):
        seqs, chunk_len, d_model = x_in.shape
        key_dim = kv_state.shape[2]
        half = key_dim // 2
        rows = chunk_len // BLOCKS
        share = rows // CHIPS
        chunk = min(CHUNK, rows)
        me = lax.axis_index('tp')
        log_gamma = jnp.log1p(-jnp.exp2(-5.0 - me.astype(F32)))
        ids = jnp.arange(chunk)
        gap = ids[:, None] - ids[None, :]
        decay = jnp.where(gap >= 0, jnp.exp(jnp.maximum(gap, 0).astype(F32) * log_gamma), 0.0)
        lane = jnp.arange(128)[None, :]
        power = jnp.where(lane == 0, ids[:, None] + 1, jnp.where(lane == 1, chunk - 1 - ids[:, None], chunk))
        edge = jnp.exp(power.astype(F32) * log_gamma)
        inv_freq = jnp.power(ROPE_BASE, -jnp.arange(half).astype(F32) / half)
        low = ids.astype(F32)[:, None] * inv_freq[None, :]
        table = jnp.stack([jnp.cos(low), jnp.sin(low)])
        high = (start_pos[:, None] + jnp.arange(chunk_len // chunk)[None, :] * chunk).astype(F32)[:, :, None] * inv_freq
        base = jnp.stack([jnp.cos(high), jnp.sin(high)], axis=2)

        anywhere = pl.BlockSpec(memory_space=pl.ANY)
        vmem = pl.BlockSpec(memory_space=pltpu.VMEM)
        dma = lambda *shape: pltpu.SemaphoreType.DMA(shape)
        out, state, _, _ = pl.pallas_call(
            layer_kernel,
            in_specs=[anywhere, vmem, vmem, vmem, vmem, vmem] + [anywhere] * 7 + [vmem] * 4,
            out_specs=[anywhere, vmem, anywhere, anywhere],
            out_shape=[
                jax.ShapeDtypeStruct((seqs, BLOCKS, CHIPS, share, d_model), BF16),
                jax.ShapeDtypeStruct(kv_state.shape, F32),
                jax.ShapeDtypeStruct((members,) + w_up.shape, BF16),
                jax.ShapeDtypeStruct((members,) + w_down.shape, BF16),
            ],
            scratch_shapes=[
                pltpu.VMEM(w_q.shape, BF16), pltpu.VMEM(w_k.shape, BF16), pltpu.VMEM(w_v.shape, BF16), pltpu.VMEM(w_g.shape, BF16),
                pltpu.VMEM(w_o.shape, BF16), pltpu.VMEM(w_down.shape, BF16),
                pltpu.VMEM((2, CHIPS, share, d_model), BF16), pltpu.VMEM((rows, d_model), BF16), pltpu.VMEM((2, rows, d_model), BF16),
                pltpu.VMEM((BLOCKS, rows, d_model), BF16), pltpu.VMEM((2, BLOCKS, CHIPS - 1, share, d_model), BF16),
                pltpu.VMEM((BLOCKS, share, d_model), BF16), pltpu.VMEM((2 * share, d_model), BF16), pltpu.VMEM((2 * share, d_model), F32),
                dma(5), dma(2), pltpu.SemaphoreType.DMA, dma(2, 2), pltpu.SemaphoreType.DMA, dma(2), pltpu.SemaphoreType.REGULAR,
                dma(2, BLOCKS, 3), dma(2, BLOCKS, 3), dma(2, 4, 2), dma(4, 2), dma(2, 4, 2), dma(2, 4, 2), dma(4, 2), dma(4, 2), dma(4, 2), dma(4, 2),
                dma(BLOCKS, 2, 4), dma(BLOCKS, 4), dma(BLOCKS, 4), dma(BLOCKS, 4), dma(BLOCKS),
            ],
            compiler_params=pltpu.CompilerParams(collective_id=0, has_side_effects=True, vmem_limit_bytes=67043328),
            name="layer",
        )(x_in.reshape(seqs, BLOCKS, CHIPS, share, d_model), kv_state, *(a[None, :] for a in (ln1_gain, ln1_bias, ln2_gain, ln2_bias)), w_q, w_k, w_v, w_g, w_o, w_up, w_down, base, table, decay, edge)
        return out.reshape(seqs, chunk_len, d_model), state

    in_specs = (P('dp', None, None), P('dp'), P('dp', 'tp', None, None), P(), P(), P(None, 'tp'), P(None, 'tp'), P(None, 'tp'), P(None, 'tp'), P('tp', None), P(), P(), P(None, 'tp'), P('tp', None))
    out_specs = (P('dp', None, None), P('dp', 'tp', None, None))
    return jax.shard_map(local_layer, mesh=mesh, in_specs=in_specs, out_specs=out_specs, check_vma=False)
```

```python
import math

import jax
import jax.numpy as jnp
from jax import lax
from jax.experimental import pallas as pl
from jax.experimental.pallas import tpu as pltpu
from jax.sharding import PartitionSpec as P

NORM_EPS = 1e-5
GROUP_EPS = 1e-6
ROPE_BASE = 10000.0
CHUNK = 256
BLOCKS = 4
CHIPS = 4
PARTS = 2
F32 = jnp.float32
BF16 = jnp.bfloat16
MESH = pl.DeviceIdType.MESH
LOOP = {
    0: (
        ('s1', 'e', 1, 0),
    ),
    1: (
        ('s1', 'e', 1, 1),
    ),
    2: (
        ('s1', 'e', 2, 0), ('s1', 'm', 'f1', 0), ('s1', 'm', 'f1', 1), ('s1', 'm', 'n1', 0), ('s1', 'm', 'n1', 1), ('s1', 'm', 'f2', 0),
    ),
    3: (
        ('rs', 'm', 0, 0, 'n'), ('s1', 'e', 2, 1),
    ),
    4: (
        ('s2', 'e', 1, 0), ('s1', 'm', 'f2', 1), ('s2', 'e', 2, 1), ('rs', 'm', 0, 1, 'n'), ('s2', 'e', 2, 0),
    ),
    5: (
        ('rs', 'm', 0, 0, 'f'), ('s1', 'e', 3, 0), ('s2', 'e', 1, 1), ('s3', 'e', 1, 0),
    ),
    6: (
        ('s3', 'e', 2, 1), ('rs', 'm', 1, 1, 'n'), ('s1', 'e', 3, 1), ('rs', 'm', 1, 0, 'n'), ('rs', 'm', 0, 1, 'f'),
        ('rs', 'm', 1, 1, 'f'),
    ),
}
BETWEEN = (
    ('rs', 'm', 2, 0, 'n'), ('s2', 'e', 3, 0), ('s2', 'e', 3, 1), ('rs', 'm', 1, 0, 'f'), ('fin', 'e', 0, 1), ('fin', 'e', 0, 0),
    ('rs', 'm', 3, 0, 'n'), ('s3', 'e', 1, 1), ('fin', 'e', 1, 1), ('rs', 'm', 2, 1, 'n'),
)
TILES = {
    2: (
        ('s3', 'e', 2, 0), ('s3', 'e', 3, 0),
    ),
    4: (
        ('s3', 'e', 3, 1), ('rs', 'm', 2, 0, 'f'),
    ),
    6: (
        ('rs', 'm', 3, 1, 'n'),
    ),
    7: (
        ('fin', 'e', 1, 0),
    ),
    9: (
        ('rs', 'm', 3, 0, 'f'), ('rs', 'm', 2, 1, 'f'),
    ),
    12: (
        ('ag', 'm', 'n', 0, 0),
    ),
    13: (
        ('fin', 'e', 3, 0),
    ),
    16: (
        ('fin', 'e', 2, 1), ('fin', 'e', 2, 0), ('rs', 'm', 3, 1, 'f'),
    ),
    18: (
        ('ag', 'm', 'n', 0, 1), ('ag', 'm', 'f', 0, 0), ('ag', 'm', 'n', 1, 0),
    ),
    19: (
        ('ag', 'm', 'f', 0, 1), ('ag', 'm', 'n', 1, 1), ('ag', 'm', 'f', 1, 0),
    ),
    20: (
        ('ag', 'm', 'n', 2, 0), ('ag', 'm', 'f', 1, 1), ('ag', 'm', 'n', 2, 1),
    ),
    23: (
        ('fin', 'e', 3, 1), ('ag', 'm', 'f', 2, 0), ('ag', 'm', 'n', 3, 0),
    ),
    25: (
        ('ag', 'e', 'x', 0, 0),
    ),
    27: (
        ('ag', 'm', 'f', 2, 1),
    ),
}
TAIL = (
    ('ag', 'm', 'n', 3, 1), ('ag', 'e', 'x', 2, 1), ('ag', 'e', 'x', 2, 0), ('ag', 'e', 'x', 1, 1), ('ag', 'm', 'f', 3, 0),
    ('ag', 'm', 'f', 3, 1), ('ag', 'e', 'x', 1, 0), ('ag', 'e', 'x', 3, 0), ('ag', 'e', 'x', 0, 1), ('ag', 'e', 'x', 3, 1),
)


def normalize(x_f32, gain, bias):
    row_mean = jnp.mean(x_f32, axis=-1, keepdims=True)
    centered = x_f32 - row_mean
    variance = jnp.mean(centered * centered, axis=-1, keepdims=True)
    return centered * lax.rsqrt(variance + NORM_EPS) * gain + bias


def add_bf16(*terms):
    return sum(t.astype(F32) for t in terms).astype(BF16)


def layer_kernel(x_any, state_in, gain1, bias1, gain2, bias2, wq_any, wk_any, wv_any, wg_any, wo_any, up_any, down_any, cos_high, sin_high, cos_low, sin_low,
                 out_any, state_ref, up_all, down_all,
                 wq, wk, wv, wg, wo, wd, x_buf, part, met, own, rs, mid, hid, acc, decay, edge,
                 load_sem, x_sem, mid_sem, tile_sem, met_s, met_r, credit, rs_s, rs_r, z_s, z_r, f_s, f_r, g_s, g_r, p_s, p_r, ag_s, ag_r, agp_s, agp_r, put_sem):
    group, me = lax.axis_index('dp'), lax.axis_index('tp')
    chip, core = lax.div(me, 2), lax.rem(me, 2)
    partner = me + 1 - 2 * core
    across_x = lax.rem(group + 2, 4)
    across_y = group + 1 - 2 * lax.rem(group, 2)
    chunk = cos_low.shape[0]
    rows, share = own.shape[1], mid.shape[1]
    key_dim, half = wq.shape[1], wq.shape[1] // 2
    last = CHIPS - 1
    far = 1 - 2 * lax.div(chip, 2)
    is_end = (chip == 0) | (chip == last)
    is_middle = (chip > 0) & (chip < last)

    def remote(src, dst, s, r, **where):
        return pltpu.make_async_remote_copy(src_ref=src, dst_ref=dst, send_sem=s, recv_sem=r, device_id=where, device_id_type=MESH)

    def side_of(flow):
        return lax.div(1 - flow, 2)

    shard = lax.div(chip, 2)
    weight_all, weight_own = (up_all, down_all), (up_any, down_any)
    quarter = tuple(w.shape[0] // 4 for w in weight_own)

    def origin_of(which):
        return {'n1': chip - far, 'f1': chip + far, 'f2': chip + 2 * far}[which] if isinstance(which, str) else chip + which * far

    def piece(p, index, q):
        return weight_all[p].at[index, pl.ds(q * quarter[p], quarter[p])]

    def z_copy(flow, origin, p, own_piece=False):
        slot = piece(p, 2 * origin + core, group)
        src = weight_own[p].at[pl.ds(group * quarter[p], quarter[p])] if own_piece else slot
        return remote(src, slot, z_s.at[side_of(flow), origin, p], z_r.at[origin, p], tp=me + 2 * flow)

    def first_copy(axis, origin, p, q=None):
        slot = piece(p, 2 * origin + core, group if q is None else q)
        return remote(slot, slot, f_s.at[axis, origin, p], f_r.at[axis, origin, p], dp=across_x if axis == 0 else across_y)

    def second_copy(origin, p, q=None):
        slot = piece(p, 2 * origin + core, (across_x if p == 0 else across_y) if q is None else q)
        return remote(slot, slot, g_s.at[origin, p], g_r.at[origin, p], dp=across_y if p == 0 else across_x)

    def partner_copy(origin, p, own_shard=False, incoming=False):
        slot = weight_all[p].at[2 * origin + (1 - core if incoming else core)]
        return remote(weight_own[p] if own_shard else slot, slot, p_s.at[origin, p], p_r.at[origin, p], tp=partner)

    def spread_first(which, p):
        origin = origin_of(which)
        z_copy(far, origin, p).wait_recv()
        if isinstance(which, str):
            z_copy(far if which == 'n1' else -far, origin, p).start()
        else:
            for axis in range(2):
                first_copy(axis, origin, p).start()

    def spread_second(which, p):
        origin = origin_of(which)
        first_copy(p, origin, p, across_x if p == 0 else across_y).wait_recv()
        second_copy(origin, p).start()

    def spread_third(which, p):
        origin = origin_of(which)
        first_copy(1 - p, origin, p, across_y if p == 0 else across_x).wait_recv()
        second_copy(origin, p, 3 - group).wait_recv()
        partner_copy(origin, p).start()

    def strip(h):
        return pl.ds(h * (share // PARTS), share // PARTS)

    def mine(i, h, side):
        return own[i, pl.ds(pl.multiple_of((1 - side) * share + h * (share // PARTS), share // PARTS), share // PARTS)]

    def rs_copy(flow, i, h, fresh=False):
        side = side_of(flow)
        slot = rs.at[side, i, strip(h)]
        src = own.at[i, pl.ds((1 - side) * share + h * (share // PARTS), share // PARTS)] if fresh else slot
        return remote(src, slot, rs_s.at[side, i, h], rs_r.at[side, i, h], tp=me + 2 * flow)

    def rs_first(i):
        @pl.when(is_end)
        def _():
            for h in range(PARTS):
                rs_copy(far, i, h, fresh=True).start()

    def rs_step(i, h, which):
        flow = far if which == 'n' else -far
        side = side_of(flow)
        rs_copy(flow, i, h).wait_recv()
        rs[side, i, strip(h)] = add_bf16(rs[side, i, strip(h)], mine(i, h, side))
        rs_copy(flow, i, h).start()

    def rs_final(i, h):
        side = side_of(-far)
        rs_copy(-far, i, h).wait_recv()
        mid[i, strip(h)] = add_bf16(mid[i, strip(h)], add_bf16(mine(i, h, side), rs[side, i, strip(h)]))

    def ag_copy(b, h, origin, fresh=False):
        slot = out_any.at[core, b, origin, strip(h)]
        return remote(mid.at[b, strip(h)] if fresh else slot, slot, ag_s.at[b, h, origin], ag_r.at[b, h, origin], tp=me + 2 * (1 - 2 * origin))

    def agp_copy(b, h, origin, fresh=False, incoming=False):
        slot = out_any.at[1 - core if incoming else core, b, origin, strip(h)]
        return remote(mid.at[b, strip(h)] if fresh else slot, slot, agp_s.at[b, h, origin], agp_r.at[b, h, origin], tp=partner)

    def put_copy(b):
        return pltpu.make_async_copy(mid.at[b], out_any.at[core, b, shard], put_sem.at[b])

    def ag_first(b):
        for h in range(PARTS):
            ag_copy(b, h, shard, fresh=True).start()
        for h in range(PARTS):
            agp_copy(b, h, shard, fresh=True).start()
        put_copy(b).start()

    def ag_step(which, b, h):
        origin = shard if which == 'n' else 1 - shard
        ag_copy(b, h, origin).wait_recv()
        if which != 'x':
            ag_copy(b, h, origin).start()
        agp_copy(b, h, origin).start()

    serves = {'s1': spread_first, 's2': spread_second, 's3': spread_third, 'rs': rs_step, 'fin': rs_final, 'ag': ag_step}

    def serve(items):
        for item in items:
            @pl.when(is_end if item[1] == 'e' else is_middle)
            def _():
                serves[item[0]](*item[2:])

    def x_copy(n):
        seq = core + (1 - 2 * core) * (1 - lax.rem(n, 2))
        return pltpu.make_async_copy(x_any.at[seq, lax.div(n, 2)], x_buf.at[lax.rem(n, 2)], x_sem.at[lax.rem(n, 2)])

    def met_copy(i):
        return remote(part, met.at[lax.rem(i, 2)], met_s, met_r.at[lax.rem(i, 2)], tp=partner)

    barrier = pltpu.get_barrier_semaphore()
    for where in ({'tp': partner}, {'dp': across_x}, {'dp': across_y}):
        pl.semaphore_signal(barrier, inc=1, device_id=where, device_id_type=MESH)

    @pl.when(chip < last)
    def _():
        pl.semaphore_signal(barrier, inc=1, device_id={'tp': me + 2}, device_id_type=MESH)

    @pl.when(chip > 0)
    def _():
        pl.semaphore_signal(barrier, inc=1, device_id={'tp': me - 2}, device_id_type=MESH)

    loads = [pltpu.make_async_copy(a, b, load_sem.at[k]) for k, (a, b) in enumerate(((wq_any, wq), (wk_any, wk), (wv_any, wv), (wg_any, wg), (wo_any, wo)))]
    x_copy(0).start()
    for load in loads:
        load.start()
    mid_load = pltpu.make_async_copy(x_any.at[core, :, shard], mid, mid_sem)
    mid_load.start()
    pl.semaphore_wait(barrier, 4 + is_middle.astype(jnp.int32))

    for p in range(2):
        z_copy(far, chip, p, own_piece=True).start()

        @pl.when(is_middle)
        def _():
            z_copy(-far, chip, p, own_piece=True).start()

        @pl.when(is_end)
        def _():
            partner_copy(chip, p, own_shard=True).start()

    state_ref[...] = state_in[...]
    log_gamma = F32(0.0)
    for head in range(2 * CHIPS):
        log_gamma = jnp.where(me == head, F32(math.log1p(-2.0 ** (-5 - head))), log_gamma)
    gap = lax.broadcasted_iota(jnp.int32, (chunk, chunk), 0) - lax.broadcasted_iota(jnp.int32, (chunk, chunk), 1)
    decay[...] = jnp.where(gap >= 0, jnp.exp(jnp.maximum(gap, 0).astype(F32) * log_gamma), 0.0)
    lane = lax.broadcasted_iota(jnp.int32, edge.shape, 1)
    ids = lax.broadcasted_iota(jnp.int32, edge.shape, 0)
    power = jnp.where(lane == 0, ids + 1, jnp.where(lane == 1, chunk - 1 - ids, chunk))
    edge[...] = jnp.exp(power.astype(F32) * log_gamma)
    for load in loads:
        load.wait()
    mid_load.wait()

    def attend(n, carry):
        i, k = lax.div(n, 2), lax.rem(n, 2)
        seq = core + (1 - 2 * core) * (1 - k)
        x_copy(n).wait()

        @pl.when(n < 2 * BLOCKS - 1)
        def _():
            x_copy(n + 1).start()

        h = normalize(x_buf[k].reshape(rows, part.shape[1]).astype(F32), gain1[...], bias1[...]).astype(BF16)
        q_raw = jnp.dot(h, wq[...], preferred_element_type=F32)
        k_raw = jnp.dot(h, wk[...], preferred_element_type=F32)
        v_all = jnp.dot(h, wv[...], preferred_element_type=F32).astype(BF16)
        g_all = jnp.dot(h, wg[...], preferred_element_type=F32)
        cos_lo, sin_lo = cos_low[...], sin_low[...]
        mixed = []
        subs = rows // chunk
        for sub in range(subs):
            span = slice(sub * chunk, (sub + 1) * chunk)
            row = pl.ds(i * subs + sub, 1)
            cos_hi, sin_hi = cos_high[seq, row, :], sin_high[seq, row, :]
            cos_t = cos_hi * cos_lo - sin_hi * sin_lo
            sin_t = sin_hi * cos_lo + cos_hi * sin_lo

            def rotate(raw):
                first, second = raw[span, :half], raw[span, half:]
                return jnp.concatenate([first * cos_t - second * sin_t, second * cos_t + first * sin_t], axis=-1)

            queries = rotate(q_raw).astype(BF16)
            keys = (rotate(k_raw) * key_dim ** -0.5).astype(BF16)
            values = v_all[span]
            state = state_ref[seq, 0]
            scores = lax.dot_general(queries, keys, (((1,), (1,)), ((), ())), preferred_element_type=F32) * decay[...]
            retained = jnp.dot(scores.astype(BF16), values, preferred_element_type=F32)
            retained += jnp.dot(queries, state.astype(BF16), preferred_element_type=F32) * edge[:, 0:1]
            keys_decayed = (keys.astype(F32) * edge[:, 1:2]).astype(BF16)
            grown = lax.dot_general(keys_decayed, values, (((0,), (0,)), ((), ())), preferred_element_type=F32)
            state_ref[seq, 0] = state * edge[0:1, 2:3] + grown
            row_mean = jnp.mean(retained, axis=-1, keepdims=True)
            centered = retained - row_mean
            variance = jnp.mean(centered * centered, axis=-1, keepdims=True)
            normed = centered * lax.rsqrt(variance + GROUP_EPS)
            mixed.append((jax.nn.silu(g_all[span]) * normed).astype(BF16))
        u = jnp.dot(jnp.concatenate(mixed, axis=0), wo[...], preferred_element_type=F32).astype(BF16)

        @pl.when(k == 1)
        def _():
            met_copy(i).wait_send()

        part[...] = u

        @pl.when(k == 0)
        def _():
            @pl.when(i >= 2)
            def _():
                pl.semaphore_wait(credit, 1)

            met_copy(i).start()

        @pl.when(k == 1)
        def _():
            met_copy(i).wait_recv()
            own[i] = add_bf16(part[...], met[lax.rem(i, 2)])

            @pl.when(i < BLOCKS - 2)
            def _():
                pl.semaphore_signal(credit, inc=1, device_id={'tp': partner}, device_id_type=MESH)

            rs_first(i)

        for turn, items in LOOP.items():
            @pl.when(n == turn)
            def _():
                serve(items)

        return carry

    lax.fori_loop(0, 2 * BLOCKS, attend, 0)

    serve(BETWEEN)

    slots = ((wv, wo), (wg, wd))

    def tile_copies(index, slot, own_shard=False):
        sources = (up_any, down_any) if own_shard else (up_all.at[index], down_all.at[index])
        return [pltpu.make_async_copy(sources[p], slots[slot][p], tile_sem.at[slot, p]) for p in range(2)]

    def ffn_tile(slot):
        for copy in tile_copies(0, slot):
            copy.wait()
        up, down = slots[slot]
        pre = jnp.dot(hid[...], up[...], preferred_element_type=F32)
        act = (0.5 * pre * (1.0 + lax.erf(pre * 0.5 ** 0.5))).astype(BF16)
        acc[...] += jnp.dot(act, down[...], preferred_element_type=F32)

    def ffn_finish(b):
        mid[b] = add_bf16(mid[b], acc[...].astype(BF16))
        ag_first(b)

    def serve_at(pair, parity, fresh):
        for turn, items in TILES.items():
            if turn % 2 == parity and (turn % 8 == 0) == fresh:
                @pl.when(pair == turn // 2)
                def _():
                    serve(items)

    def ffn_pair(pair, carry):
        b, e = lax.div(pair, CHIPS), lax.rem(pair, CHIPS)
        index = 2 * (chip + e * far) + core
        serve_at(pair, 0, False)

        @pl.when(is_end)
        def _():
            @pl.when(e == 0)
            def _():
                for copy in tile_copies(index, 0, own_shard=True):
                    copy.start()

            @pl.when(e > 0)
            def _():
                for copy in tile_copies(index, 0):
                    copy.start()

            @pl.when(pair > 0)
            def _():
                ffn_tile(1)

                @pl.when(e == 0)
                def _():
                    ffn_finish(b - 1)

        serve_at(pair, 0, True)

        @pl.when(is_end & (e == 0))
        def _():
            hid[...] = normalize(mid[b].astype(F32), gain2[...], bias2[...]).astype(BF16)
            acc[...] = jnp.zeros_like(acc)

        serve_at(pair, 1, False)

        @pl.when(is_end)
        def _():
            @pl.when(b == 0)
            def _():
                for p in range(2):
                    partner_copy(chip + e * far, p, incoming=True).wait_recv()

            for copy in tile_copies(index + 1 - 2 * core, 1):
                copy.start()
            ffn_tile(0)

        return carry

    lax.fori_loop(0, BLOCKS * CHIPS, ffn_pair, 0)

    @pl.when(is_end)
    def _():
        ffn_tile(1)
        ffn_finish(BLOCKS - 1)

    serve(TAIL)

    strips = [(b, h) for b in range(BLOCKS) for h in range(PARTS)]
    for b, h in strips:
        for origin in range(2):
            agp_copy(b, h, origin).wait_send()
            agp_copy(b, h, origin, incoming=True).wait_recv()
    for p in range(2):
        z_copy(far, chip, p).wait_send()

    @pl.when(is_end)
    def _():
        for b in range(BLOCKS):
            put_copy(b).wait()
        for b, h in strips:
            ag_copy(b, h, shard).wait_send()
            rs_copy(far, b, h, fresh=True).wait_send()
        for p in range(2):
            partner_copy(chip, p, own_shard=True).wait_send()
            for which in range(1, CHIPS):
                origin = origin_of(which)
                partner_copy(origin, p).wait_send()
                second_copy(origin, p).wait_send()
                for axis in range(2):
                    first_copy(axis, origin, p).wait_send()

    @pl.when(is_middle)
    def _():
        for p in range(2):
            z_copy(-far, chip, p).wait_send()
            z_copy(far, origin_of('n1'), p).wait_send()
            z_copy(-far, origin_of('f1'), p).wait_send()
            z_copy(-far, origin_of('f2'), p).wait_send()
        for b, h in strips:
            for side in range(2):
                rs_copy(1 - 2 * side, b, h).wait_send()
                ag_copy(b, h, side).wait_send()


def copy_kernel(a_ref, b_ref, a_out, b_out):
    a_out[...] = a_ref[...]
    b_out[...] = b_ref[...]


def copy_out(a, b):
    spec = pl.BlockSpec((1, a.shape[1] // 2) + a.shape[2:], lambda i: (i // 2, i % 2, 0))
    part = pl.BlockSpec((1, 1, b.shape[2] // 2, b.shape[3]), lambda i: (i // 2, 0, i % 2, 0))
    return pl.pallas_call(
        copy_kernel,
        grid=(2 * a.shape[0],),
        in_specs=[spec, part],
        out_specs=[spec, part],
        out_shape=[jax.ShapeDtypeStruct(a.shape, a.dtype), jax.ShapeDtypeStruct(b.shape, b.dtype)],
        compiler_params=pltpu.CompilerParams(vmem_limit_bytes=48 * 2 ** 20),
        name="copy_out",
    )(a, b)


def solution(mesh):
    members = mesh.shape['tp']

    def local_layer(x_in, start_pos, kv_state, ln1_gain, ln1_bias, w_q, w_k, w_v, w_g, w_o, ln2_gain, ln2_bias, w_up, w_down):
        seqs, chunk_len, d_model = x_in.shape
        key_dim = kv_state.shape[2]
        half = key_dim // 2
        rows = chunk_len // BLOCKS
        share = rows // 2
        chunk = min(CHUNK, rows)
        inv_freq = jnp.power(ROPE_BASE, -jnp.arange(half).astype(F32) / half)
        low = jnp.arange(chunk).astype(F32)[:, None] * inv_freq[None, :]
        high = (start_pos[:, None] + jnp.arange(chunk_len // chunk)[None, :] * chunk).astype(F32)[:, :, None] * inv_freq

        anywhere = pl.BlockSpec(memory_space=pl.ANY)
        vmem = pl.BlockSpec(memory_space=pltpu.VMEM)
        dma = lambda *shape: pltpu.SemaphoreType.DMA(shape)
        out, state, _, _ = pl.pallas_call(
            layer_kernel,
            in_specs=[anywhere, vmem, vmem, vmem, vmem, vmem] + [anywhere] * 7 + [vmem] * 4,
            out_specs=[anywhere, vmem, anywhere, anywhere],
            out_shape=[
                jax.ShapeDtypeStruct((seqs, BLOCKS, 2, share, d_model), BF16),
                jax.ShapeDtypeStruct(kv_state.shape, F32),
                jax.ShapeDtypeStruct((members,) + w_up.shape, BF16),
                jax.ShapeDtypeStruct((members,) + w_down.shape, BF16),
            ],
            scratch_shapes=[
                pltpu.VMEM(w_q.shape, BF16), pltpu.VMEM(w_k.shape, BF16), pltpu.VMEM(w_v.shape, BF16), pltpu.VMEM(w_g.shape, BF16),
                pltpu.VMEM(w_o.shape, BF16), pltpu.VMEM(w_down.shape, BF16),
                pltpu.VMEM((2, 2, share, d_model), BF16), pltpu.VMEM((rows, d_model), BF16), pltpu.VMEM((2, rows, d_model), BF16),
                pltpu.VMEM((BLOCKS, rows, d_model), BF16), pltpu.VMEM((2, BLOCKS, share, d_model), BF16),
                pltpu.VMEM((BLOCKS, share, d_model), BF16), pltpu.VMEM((share, d_model), BF16), pltpu.VMEM((share, d_model), F32),
                pltpu.VMEM((chunk, chunk), F32), pltpu.VMEM((chunk, 128), F32),
                dma(5), dma(2), pltpu.SemaphoreType.DMA, dma(2, 2), pltpu.SemaphoreType.DMA, dma(2), pltpu.SemaphoreType.REGULAR,
                dma(2, BLOCKS, PARTS), dma(2, BLOCKS, PARTS), dma(2, 4, 2), dma(4, 2), dma(2, 4, 2), dma(2, 4, 2), dma(4, 2), dma(4, 2), dma(4, 2), dma(4, 2),
                dma(BLOCKS, PARTS, 2), dma(BLOCKS, PARTS, 2), dma(BLOCKS, PARTS, 2), dma(BLOCKS, PARTS, 2), dma(BLOCKS),
            ],
            compiler_params=pltpu.CompilerParams(collective_id=0, has_side_effects=True, vmem_limit_bytes=67043328),
            name="layer",
        )(x_in.reshape(seqs, BLOCKS, 2, share, d_model), kv_state, *(a[None, :] for a in (ln1_gain, ln1_bias, ln2_gain, ln2_bias)), w_q, w_k, w_v, w_g, w_o, w_up, w_down, jnp.cos(high), jnp.sin(high), jnp.cos(low), jnp.sin(low))
        return copy_out(out.reshape(seqs, chunk_len, d_model), state)

    in_specs = (P('dp', None, None), P('dp'), P('dp', 'tp', None, None), P(), P(), P(None, 'tp'), P(None, 'tp'), P(None, 'tp'), P(None, 'tp'), P('tp', None), P(), P(), P(None, 'tp'), P('tp', None))
    out_specs = (P('dp', None, None), P('dp', 'tp', None, None))
    return jax.shard_map(local_layer, mesh=mesh, in_specs=in_specs, out_specs=out_specs, check_vma=False)
```

```python
import math

import jax
import jax.numpy as jnp
from jax import lax
from jax.experimental import pallas as pl
from jax.experimental.pallas import tpu as pltpu
from jax.sharding import PartitionSpec as P

NORM_EPS = 1e-5
GROUP_EPS = 1e-6
ROPE_BASE = 10000.0
CHUNK = 256
LOW = 16
BLOCKS = 4
CHIPS = 4
PARTS = 2
F32 = jnp.float32
BF16 = jnp.bfloat16
MESH = pl.DeviceIdType.MESH
LOOP = {
    0: (
        ('s1', 'e', 1, 0),
    ),
    1: (
        ('s1', 'e', 1, 1),
    ),
    2: (
        ('s1', 'e', 2, 0), ('s1', 'm', 'f1', 0), ('s1', 'm', 'f1', 1), ('s1', 'm', 'n1', 0), ('s1', 'm', 'n1', 1), ('s1', 'm', 'f2', 0),
    ),
    3: (
        ('rs', 'm', 0, 0, 'n'), ('s1', 'e', 2, 1),
    ),
    4: (
        ('s2', 'e', 1, 0), ('s1', 'm', 'f2', 1), ('s2', 'e', 2, 1), ('rs', 'm', 0, 1, 'n'), ('s2', 'e', 2, 0),
    ),
    5: (
        ('rs', 'm', 0, 0, 'f'), ('s1', 'e', 3, 0), ('s2', 'e', 1, 1), ('s3', 'e', 1, 0),
    ),
    6: (
        ('s3', 'e', 2, 1), ('rs', 'm', 1, 1, 'n'), ('s1', 'e', 3, 1), ('rs', 'm', 1, 0, 'n'), ('rs', 'm', 0, 1, 'f'),
        ('rs', 'm', 1, 1, 'f'),
    ),
}
BETWEEN = (
    ('rs', 'm', 2, 0, 'n'), ('s2', 'e', 3, 0), ('s2', 'e', 3, 1), ('rs', 'm', 1, 0, 'f'), ('fin', 'e', 0, 1), ('fin', 'e', 0, 0),
    ('rs', 'm', 3, 0, 'n'), ('s3', 'e', 1, 1), ('fin', 'e', 1, 1), ('rs', 'm', 2, 1, 'n'),
)
TILES = {
    2: (
        ('s3', 'e', 2, 0), ('s3', 'e', 3, 0),
    ),
    4: (
        ('s3', 'e', 3, 1), ('rs', 'm', 2, 0, 'f'),
    ),
    6: (
        ('rs', 'm', 3, 1, 'n'),
    ),
    7: (
        ('fin', 'e', 1, 0),
    ),
    9: (
        ('rs', 'm', 3, 0, 'f'), ('rs', 'm', 2, 1, 'f'),
    ),
    12: (
        ('ag', 'm', 'n', 0, 0),
    ),
    13: (
        ('fin', 'e', 3, 0),
    ),
    16: (
        ('fin', 'e', 2, 1), ('fin', 'e', 2, 0), ('rs', 'm', 3, 1, 'f'),
    ),
    18: (
        ('ag', 'm', 'n', 0, 1), ('ag', 'm', 'f', 0, 0), ('ag', 'm', 'n', 1, 0),
    ),
    19: (
        ('ag', 'm', 'f', 0, 1), ('ag', 'm', 'n', 1, 1), ('ag', 'm', 'f', 1, 0),
    ),
    20: (
        ('ag', 'm', 'n', 2, 0), ('ag', 'm', 'f', 1, 1), ('ag', 'm', 'n', 2, 1),
    ),
    23: (
        ('fin', 'e', 3, 1), ('ag', 'm', 'f', 2, 0), ('ag', 'm', 'n', 3, 0),
    ),
    25: (
        ('ag', 'e', 'x', 0, 0),
    ),
    27: (
        ('ag', 'm', 'f', 2, 1),
    ),
}
TAIL = (
    ('ag', 'm', 'n', 3, 1), ('ag', 'e', 'x', 2, 1), ('ag', 'e', 'x', 2, 0), ('ag', 'e', 'x', 1, 1), ('ag', 'm', 'f', 3, 0),
    ('ag', 'm', 'f', 3, 1), ('ag', 'e', 'x', 1, 0), ('ag', 'e', 'x', 3, 0), ('ag', 'e', 'x', 0, 1), ('ag', 'e', 'x', 3, 1),
)


def normalize(x_f32, gain, bias):
    row_mean = jnp.mean(x_f32, axis=-1, keepdims=True)
    centered = x_f32 - row_mean
    variance = jnp.mean(centered * centered, axis=-1, keepdims=True)
    return centered * lax.rsqrt(variance + NORM_EPS) * gain + bias


def add_bf16(*terms):
    return sum(t.astype(F32) for t in terms).astype(BF16)


def layer_kernel(x_any, state_in, gain1, bias1, gain2, bias2, wq_any, wk_any, wv_any, wg_any, wo_any, up_any, down_any, cos_rows, sin_rows,
                 out_any, state_ref, up_all, down_all,
                 wq, wk, wv, wg, wo, x_buf, part, met, own, rs, hid, acc, decay, edge, cos_low, sin_low,
                 load_sem, x_sem, mid_sem, state_sem, tile_sem, met_s, met_r, credit, rs_s, rs_r, z_s, z_r, f_s, f_r, g_s, g_r, p_s, p_r, ag_s, ag_r, agp_s, agp_r, put_sem):
    group, me = lax.axis_index('dp'), lax.axis_index('tp')
    chip, core = lax.div(me, 2), lax.rem(me, 2)
    partner = me + 1 - 2 * core
    across_x = lax.rem(group + 2, 4)
    across_y = group + 1 - 2 * lax.rem(group, 2)
    chunk = decay.shape[0]
    rows, share = own.shape[1], rs.shape[2]
    key_dim, half = wq.shape[1], wq.shape[1] // 2
    last = CHIPS - 1
    far = 1 - 2 * lax.div(chip, 2)
    is_end = (chip == 0) | (chip == last)
    is_middle = (chip > 0) & (chip < last)

    def remote(src, dst, s, r, **where):
        return pltpu.make_async_remote_copy(src_ref=src, dst_ref=dst, send_sem=s, recv_sem=r, device_id=where, device_id_type=MESH)

    def side_of(flow):
        return lax.div(1 - flow, 2)

    shard, kept = lax.div(chip, 2), side_of(far)
    weight_all, weight_own = (up_all, down_all), (up_any, down_any)
    quarter = tuple(w.shape[0] // 4 for w in weight_own)

    def origin_of(which):
        return {'n1': chip - far, 'f1': chip + far, 'f2': chip + 2 * far}[which] if isinstance(which, str) else chip + which * far

    def piece(p, index, q):
        return weight_all[p].at[index, pl.ds(q * quarter[p], quarter[p])]

    def z_copy(flow, origin, p, own_piece=False):
        slot = piece(p, 2 * origin + core, group)
        src = weight_own[p].at[pl.ds(group * quarter[p], quarter[p])] if own_piece else slot
        return remote(src, slot, z_s.at[side_of(flow), origin, p], z_r.at[origin, p], tp=me + 2 * flow)

    def first_copy(axis, origin, p, q=None):
        slot = piece(p, 2 * origin + core, group if q is None else q)
        return remote(slot, slot, f_s.at[axis, origin, p], f_r.at[axis, origin, p], dp=across_x if axis == 0 else across_y)

    def second_copy(origin, p, q=None):
        slot = piece(p, 2 * origin + core, (across_x if p == 0 else across_y) if q is None else q)
        return remote(slot, slot, g_s.at[origin, p], g_r.at[origin, p], dp=across_y if p == 0 else across_x)

    def partner_copy(origin, p, own_shard=False, incoming=False):
        slot = weight_all[p].at[2 * origin + (1 - core if incoming else core)]
        return remote(weight_own[p] if own_shard else slot, slot, p_s.at[origin, p], p_r.at[origin, p], tp=partner)

    def spread_first(which, p):
        origin = origin_of(which)
        z_copy(far, origin, p).wait_recv()
        if isinstance(which, str):
            z_copy(far if which == 'n1' else -far, origin, p).start()
        else:
            for axis in range(2):
                first_copy(axis, origin, p).start()

    def spread_second(which, p):
        origin = origin_of(which)
        first_copy(p, origin, p, across_x if p == 0 else across_y).wait_recv()
        second_copy(origin, p).start()

    def spread_third(which, p):
        origin = origin_of(which)
        first_copy(1 - p, origin, p, across_y if p == 0 else across_x).wait_recv()
        second_copy(origin, p, 3 - group).wait_recv()
        partner_copy(origin, p).start()

    def strip(h):
        return pl.ds(h * (share // PARTS), share // PARTS)

    def mine(i, h, side):
        return own[i, pl.ds(pl.multiple_of((1 - side) * share + h * (share // PARTS), share // PARTS), share // PARTS)]

    def rs_copy(flow, i, h, fresh=False):
        side = side_of(flow)
        slot = rs.at[side, i, strip(h)]
        src = own.at[i, pl.ds((1 - side) * share + h * (share // PARTS), share // PARTS)] if fresh else slot
        return remote(src, slot, rs_s.at[side, i, h], rs_r.at[side, i, h], tp=me + 2 * flow)

    def rs_first(i):
        @pl.when(is_end)
        def _():
            for h in range(PARTS):
                rs_copy(far, i, h, fresh=True).start()

    def rs_step(i, h, which):
        flow = far if which == 'n' else -far
        side = side_of(flow)
        rs_copy(flow, i, h).wait_recv()
        rs[side, i, strip(h)] = add_bf16(rs[side, i, strip(h)], mine(i, h, side))
        rs_copy(flow, i, h).start()

    def rs_final(i, h):
        side = side_of(-far)
        rs_copy(-far, i, h).wait_recv()
        rs[kept, i, strip(h)] = add_bf16(rs[kept, i, strip(h)], add_bf16(mine(i, h, side), rs[side, i, strip(h)]))

    def ag_copy(b, h, origin, fresh=False):
        slot = out_any.at[core, b, origin, strip(h)]
        return remote(rs.at[kept, b, strip(h)] if fresh else slot, slot, ag_s.at[b, h, origin], ag_r.at[b, h, origin], tp=me + 2 * (1 - 2 * origin))

    def agp_copy(b, h, origin, fresh=False, incoming=False):
        slot = out_any.at[1 - core if incoming else core, b, origin, strip(h)]
        return remote(rs.at[kept, b, strip(h)] if fresh else slot, slot, agp_s.at[b, h, origin], agp_r.at[b, h, origin], tp=partner)

    def put_copy(b):
        return pltpu.make_async_copy(rs.at[kept, b], out_any.at[core, b, shard], put_sem.at[b])

    def ag_first(b):
        for h in range(PARTS):
            ag_copy(b, h, shard, fresh=True).start()
        for h in range(PARTS):
            agp_copy(b, h, shard, fresh=True).start()
        put_copy(b).start()

    def ag_step(which, b, h):
        origin = shard if which == 'n' else 1 - shard
        ag_copy(b, h, origin).wait_recv()
        if which != 'x':
            ag_copy(b, h, origin).start()
        agp_copy(b, h, origin).start()

    serves = {'s1': spread_first, 's2': spread_second, 's3': spread_third, 'rs': rs_step, 'fin': rs_final, 'ag': ag_step}

    def serve(items):
        for item in items:
            @pl.when(is_end if item[1] == 'e' else is_middle)
            def _():
                serves[item[0]](*item[2:])

    def x_copy(n):
        seq = core + (1 - 2 * core) * (1 - lax.rem(n, 2))
        return pltpu.make_async_copy(x_any.at[seq, lax.div(n, 2)], x_buf, x_sem)

    def met_copy():
        return remote(part, met, met_s, met_r, tp=partner)

    barrier = pltpu.get_barrier_semaphore()
    for where in ({'tp': partner}, {'dp': across_x}, {'dp': across_y}):
        pl.semaphore_signal(barrier, inc=1, device_id=where, device_id_type=MESH)

    @pl.when(chip < last)
    def _():
        pl.semaphore_signal(barrier, inc=1, device_id={'tp': me + 2}, device_id_type=MESH)

    @pl.when(chip > 0)
    def _():
        pl.semaphore_signal(barrier, inc=1, device_id={'tp': me - 2}, device_id_type=MESH)

    loads = [pltpu.make_async_copy(a, b, load_sem.at[k]) for k, (a, b) in enumerate(((wq_any, wq), (wk_any, wk), (wv_any, wv), (wg_any, wg), (wo_any, wo)))]
    x_copy(0).start()
    for load in loads:
        load.start()
    state_load = pltpu.make_async_copy(state_in, state_ref, state_sem)
    state_load.start()
    mid_load = pltpu.make_async_copy(x_any.at[core, :, shard], rs.at[kept], mid_sem)

    @pl.when(is_end)
    def _():
        mid_load.start()

    pl.semaphore_wait(barrier, 4 + is_middle.astype(jnp.int32))

    for p in range(2):
        z_copy(far, chip, p, own_piece=True).start()

        @pl.when(is_middle)
        def _():
            z_copy(-far, chip, p, own_piece=True).start()

        @pl.when(is_end)
        def _():
            partner_copy(chip, p, own_shard=True).start()

    log_gamma = F32(0.0)
    for head in range(2 * CHIPS):
        log_gamma = jnp.where(me == head, F32(math.log1p(-2.0 ** (-5 - head))), log_gamma)
    gap = lax.broadcasted_iota(jnp.int32, (chunk, chunk), 0) - lax.broadcasted_iota(jnp.int32, (chunk, chunk), 1)
    decay[...] = jnp.where(gap >= 0, jnp.exp(jnp.maximum(gap, 0).astype(F32) * log_gamma), 0.0)
    lane = lax.broadcasted_iota(jnp.int32, edge.shape, 1)
    ids = lax.broadcasted_iota(jnp.int32, edge.shape, 0)
    power = jnp.where(lane == 0, ids + 1, jnp.where(lane == 1, chunk - 1 - ids, chunk))
    edge[...] = jnp.exp(power.astype(F32) * log_gamma)
    for group_row in range(chunk // LOW):
        row, span = slice(cos_rows.shape[0] - LOW - chunk // LOW + group_row, cos_rows.shape[0] - LOW - chunk // LOW + group_row + 1), slice(group_row * LOW, (group_row + 1) * LOW)
        cos_a, sin_a, cos_b, sin_b = cos_rows[row, :], sin_rows[row, :], cos_rows[cos_rows.shape[0] - LOW:, :], sin_rows[cos_rows.shape[0] - LOW:, :]
        cos_low[span, :] = cos_a * cos_b - sin_a * sin_b
        sin_low[span, :] = sin_a * cos_b + cos_a * sin_b
    for load in loads:
        load.wait()
    state_load.wait()

    @pl.when(is_end)
    def _():
        mid_load.wait()


    def attend(n, carry):
        i, k = lax.div(n, 2), lax.rem(n, 2)
        seq = core + (1 - 2 * core) * (1 - k)
        x_copy(n).wait()

        h = normalize(x_buf[...].reshape(rows, part.shape[1]).astype(F32), gain1[...], bias1[...]).astype(BF16)

        @pl.when(n < 2 * BLOCKS - 1)
        def _():
            x_copy(n + 1).start()

        q_raw = jnp.dot(h, wq[...], preferred_element_type=F32)
        k_raw = jnp.dot(h, wk[...], preferred_element_type=F32)
        v_all = jnp.dot(h, wv[...], preferred_element_type=F32).astype(BF16)
        g_all = jnp.dot(h, wg[...], preferred_element_type=F32)
        cos_lo, sin_lo = cos_low[...], sin_low[...]
        mixed = []
        subs = rows // chunk
        for sub in range(subs):
            span = slice(sub * chunk, (sub + 1) * chunk)
            row = pl.ds(seq * (BLOCKS * subs) + i * subs + sub, 1)
            cos_hi, sin_hi = cos_rows[row, :], sin_rows[row, :]
            cos_t = cos_hi * cos_lo - sin_hi * sin_lo
            sin_t = sin_hi * cos_lo + cos_hi * sin_lo

            def rotate(raw):
                first, second = raw[span, :half], raw[span, half:]
                return jnp.concatenate([first * cos_t - second * sin_t, second * cos_t + first * sin_t], axis=-1)

            queries = rotate(q_raw).astype(BF16)
            keys = (rotate(k_raw) * key_dim ** -0.5).astype(BF16)
            values = v_all[span]
            state = state_ref[seq, 0]
            scores = lax.dot_general(queries, keys, (((1,), (1,)), ((), ())), preferred_element_type=F32) * decay[...]
            retained = jnp.dot(scores.astype(BF16), values, preferred_element_type=F32)
            retained += jnp.dot(queries, state.astype(BF16), preferred_element_type=F32) * edge[:, 0:1]
            keys_decayed = (keys.astype(F32) * edge[:, 1:2]).astype(BF16)
            grown = lax.dot_general(keys_decayed, values, (((0,), (0,)), ((), ())), preferred_element_type=F32)
            state_ref[seq, 0] = state * edge[0:1, 2:3] + grown
            row_mean = jnp.mean(retained, axis=-1, keepdims=True)
            centered = retained - row_mean
            variance = jnp.mean(centered * centered, axis=-1, keepdims=True)
            normed = centered * lax.rsqrt(variance + GROUP_EPS)
            mixed.append((jax.nn.silu(g_all[span]) * normed).astype(BF16))
        u = jnp.dot(jnp.concatenate(mixed, axis=0), wo[...], preferred_element_type=F32).astype(BF16)

        @pl.when(k == 1)
        def _():
            met_copy().wait_send()

        part[...] = u

        @pl.when(k == 0)
        def _():
            @pl.when(i >= 1)
            def _():
                pl.semaphore_wait(credit, 1)

            met_copy().start()

        @pl.when(k == 1)
        def _():
            met_copy().wait_recv()
            own[i] = add_bf16(part[...], met[...])

            @pl.when(i < BLOCKS - 1)
            def _():
                pl.semaphore_signal(credit, inc=1, device_id={'tp': partner}, device_id_type=MESH)

            rs_first(i)

        for turn, items in LOOP.items():
            @pl.when(n == turn)
            def _():
                serve(items)

        return carry

    lax.fori_loop(0, 2 * BLOCKS, attend, 0)

    serve(BETWEEN)

    slots = ((wv, wo), (wg, part))

    def tile_copies(index, slot, own_shard=False):
        sources = (up_any, down_any) if own_shard else (up_all.at[index], down_all.at[index])
        return [pltpu.make_async_copy(sources[p], slots[slot][p], tile_sem.at[slot, p]) for p in range(2)]

    def ffn_tile(slot):
        for copy in tile_copies(0, slot):
            copy.wait()
        up, down = slots[slot]
        pre = jnp.dot(hid[...], up[...], preferred_element_type=F32)
        act = (0.5 * pre * (1.0 + lax.erf(pre * 0.5 ** 0.5))).astype(BF16)
        acc[...] += jnp.dot(act, down[...], preferred_element_type=F32)

    def ffn_finish(b):
        rs[kept, b] = add_bf16(rs[kept, b], acc[...].astype(BF16))
        ag_first(b)

    def serve_at(pair, parity, fresh):
        for turn, items in TILES.items():
            if turn % 2 == parity and (turn % 8 == 0) == fresh:
                @pl.when(pair == turn // 2)
                def _():
                    serve(items)

    def ffn_pair(pair, carry):
        b, e = lax.div(pair, CHIPS), lax.rem(pair, CHIPS)
        index = 2 * (chip + e * far) + core
        serve_at(pair, 0, False)

        @pl.when(is_end)
        def _():
            @pl.when(e == 0)
            def _():
                for copy in tile_copies(index, 0, own_shard=True):
                    copy.start()

            @pl.when(e > 0)
            def _():
                for copy in tile_copies(index, 0):
                    copy.start()

            @pl.when(pair > 0)
            def _():
                ffn_tile(1)

                @pl.when(e == 0)
                def _():
                    ffn_finish(b - 1)

        serve_at(pair, 0, True)

        @pl.when(is_end & (e == 0))
        def _():
            hid[...] = normalize(rs[kept, b].astype(F32), gain2[...], bias2[...]).astype(BF16)
            acc[...] = jnp.zeros_like(acc)

        serve_at(pair, 1, False)

        @pl.when(is_end)
        def _():
            @pl.when(b == 0)
            def _():
                for p in range(2):
                    partner_copy(chip + e * far, p, incoming=True).wait_recv()

            for copy in tile_copies(index + 1 - 2 * core, 1):
                copy.start()
            ffn_tile(0)

        return carry

    lax.fori_loop(0, BLOCKS * CHIPS, ffn_pair, 0)

    @pl.when(is_end)
    def _():
        ffn_tile(1)
        ffn_finish(BLOCKS - 1)

    serve(TAIL)

    strips = [(b, h) for b in range(BLOCKS) for h in range(PARTS)]
    for b, h in strips:
        for origin in range(2):
            agp_copy(b, h, origin).wait_send()
            agp_copy(b, h, origin, incoming=True).wait_recv()
    for p in range(2):
        z_copy(far, chip, p).wait_send()

    @pl.when(is_end)
    def _():
        for b in range(BLOCKS):
            put_copy(b).wait()
        for b, h in strips:
            ag_copy(b, h, shard).wait_send()
            rs_copy(far, b, h, fresh=True).wait_send()
        for p in range(2):
            partner_copy(chip, p, own_shard=True).wait_send()
            for which in range(1, CHIPS):
                origin = origin_of(which)
                partner_copy(origin, p).wait_send()
                second_copy(origin, p).wait_send()
                for axis in range(2):
                    first_copy(axis, origin, p).wait_send()

    @pl.when(is_middle)
    def _():
        for p in range(2):
            z_copy(-far, chip, p).wait_send()
            z_copy(far, origin_of('n1'), p).wait_send()
            z_copy(-far, origin_of('f1'), p).wait_send()
            z_copy(-far, origin_of('f2'), p).wait_send()
        for b, h in strips:
            for side in range(2):
                rs_copy(1 - 2 * side, b, h).wait_send()
                ag_copy(b, h, side).wait_send()


def solution(mesh):
    members = mesh.shape['tp']

    def local_layer(x_in, start_pos, kv_state, ln1_gain, ln1_bias, w_q, w_k, w_v, w_g, w_o, ln2_gain, ln2_bias, w_up, w_down):
        seqs, chunk_len, d_model = x_in.shape
        key_dim = kv_state.shape[2]
        half = key_dim // 2
        rows = chunk_len // BLOCKS
        share = rows // 2
        chunk = min(CHUNK, rows)
        inv_freq = jnp.power(ROPE_BASE, -jnp.arange(half).astype(F32) / half)
        pieces = chunk_len // chunk
        row = jnp.arange(seqs * pieces + chunk // LOW + LOW)
        begin = jnp.where(row < pieces, start_pos[0], start_pos[1] - pieces * chunk)
        position = jnp.where(row < seqs * pieces, begin + row * chunk, jnp.where(row < row.size - LOW, (row - seqs * pieces) * LOW, row - (row.size - LOW)))
        angles = position.astype(F32)[:, None] * inv_freq[None, :]

        anywhere = pl.BlockSpec(memory_space=pl.ANY)
        vmem = pl.BlockSpec(memory_space=pltpu.VMEM)
        dma = lambda *shape: pltpu.SemaphoreType.DMA(shape)
        out, state, _, _ = pl.pallas_call(
            layer_kernel,
            in_specs=[anywhere, anywhere, vmem, vmem, vmem, vmem] + [anywhere] * 7 + [vmem] * 2,
            out_specs=[anywhere, vmem, anywhere, anywhere],
            out_shape=[
                pltpu.VMEM((seqs, BLOCKS, 2, share, d_model), BF16),
                jax.ShapeDtypeStruct(kv_state.shape, F32),
                jax.ShapeDtypeStruct((members,) + w_up.shape, BF16),
                jax.ShapeDtypeStruct((members,) + w_down.shape, BF16),
            ],
            scratch_shapes=[
                pltpu.VMEM(w_q.shape, BF16), pltpu.VMEM(w_k.shape, BF16), pltpu.VMEM(w_v.shape, BF16), pltpu.VMEM(w_g.shape, BF16),
                pltpu.VMEM(w_o.shape, BF16),
                pltpu.VMEM((2, share, d_model), BF16), pltpu.VMEM((rows, d_model), BF16), pltpu.VMEM((rows, d_model), BF16),
                pltpu.VMEM((BLOCKS, rows, d_model), BF16), pltpu.VMEM((2, BLOCKS, share, d_model), BF16),
                pltpu.VMEM((share, d_model), BF16), pltpu.VMEM((share, d_model), F32),
                pltpu.VMEM((chunk, chunk), F32), pltpu.VMEM((chunk, 128), F32), pltpu.VMEM((chunk, half), F32), pltpu.VMEM((chunk, half), F32),
                dma(5), pltpu.SemaphoreType.DMA, pltpu.SemaphoreType.DMA, pltpu.SemaphoreType.DMA, dma(2, 2), pltpu.SemaphoreType.DMA, pltpu.SemaphoreType.DMA, pltpu.SemaphoreType.REGULAR,
                dma(2, BLOCKS, PARTS), dma(2, BLOCKS, PARTS), dma(2, 4, 2), dma(4, 2), dma(2, 4, 2), dma(2, 4, 2), dma(4, 2), dma(4, 2), dma(4, 2), dma(4, 2),
                dma(BLOCKS, PARTS, 2), dma(BLOCKS, PARTS, 2), dma(BLOCKS, PARTS, 2), dma(BLOCKS, PARTS, 2), dma(BLOCKS),
            ],
            compiler_params=pltpu.CompilerParams(collective_id=0, has_side_effects=True, vmem_limit_bytes=47 * 2 ** 20),
            name="layer",
        )(x_in.reshape(seqs, BLOCKS, 2, share, d_model), kv_state, *(a[None, :] for a in (ln1_gain, ln1_bias, ln2_gain, ln2_bias)), w_q, w_k, w_v, w_g, w_o, w_up, w_down, jnp.cos(angles), jnp.sin(angles))
        return out.reshape(seqs, chunk_len, d_model), state

    in_specs = (P('dp', None, None), P('dp'), P('dp', 'tp', None, None), P(), P(), P(None, 'tp'), P(None, 'tp'), P(None, 'tp'), P(None, 'tp'), P('tp', None), P(), P(), P(None, 'tp'), P('tp', None))
    out_specs = (P('dp', None, None), P('dp', 'tp', None, None))
    return jax.shard_map(local_layer, mesh=mesh, in_specs=in_specs, out_specs=out_specs, check_vma=False)
```

```python
import math

import jax
import jax.numpy as jnp
import numpy as np
from jax import lax
from jax.experimental import pallas as pl
from jax.experimental.pallas import tpu as pltpu
from jax.sharding import PartitionSpec as P

NORM_EPS = 1e-5
GROUP_EPS = 1e-6
ROPE_BASE = 10000.0
CHUNK = 256
LOW = 16
BLOCKS = 4
CHIPS = 4
PARTS = 2
F32 = jnp.float32
BF16 = jnp.bfloat16
MESH = pl.DeviceIdType.MESH
LOOP = {
    0: (
        ('s1', 'e', 1, 0),
    ),
    1: (
        ('s1', 'e', 1, 1),
    ),
    2: (
        ('s1', 'e', 2, 0), ('s1', 'm', 'f1', 0), ('s1', 'm', 'f1', 1), ('s1', 'm', 'n1', 0), ('s1', 'm', 'n1', 1), ('s1', 'm', 'f2', 0),
    ),
    3: (
        ('rs', 'm', 0, 0, 'n'), ('s1', 'e', 2, 1),
    ),
    4: (
        ('s2', 'e', 1, 0), ('s1', 'm', 'f2', 1), ('s2', 'e', 2, 1), ('rs', 'm', 0, 1, 'n'), ('s2', 'e', 2, 0),
    ),
    5: (
        ('rs', 'm', 0, 0, 'f'), ('s1', 'e', 3, 0), ('s2', 'e', 1, 1), ('s3', 'e', 1, 0),
    ),
    6: (
        ('s3', 'e', 2, 1), ('rs', 'm', 1, 1, 'n'), ('s1', 'e', 3, 1), ('rs', 'm', 1, 0, 'n'), ('rs', 'm', 0, 1, 'f'),
        ('rs', 'm', 1, 1, 'f'),
    ),
}
BETWEEN = (
    ('rs', 'm', 2, 0, 'n'), ('s2', 'e', 3, 0), ('s2', 'e', 3, 1), ('rs', 'm', 1, 0, 'f'), ('fin', 'e', 0, 1), ('fin', 'e', 0, 0),
    ('rs', 'm', 3, 0, 'n'), ('s3', 'e', 1, 1), ('fin', 'e', 1, 1), ('rs', 'm', 2, 1, 'n'),
)
TILES = {
    2: (
        ('s3', 'e', 2, 0), ('s3', 'e', 3, 0),
    ),
    4: (
        ('s3', 'e', 3, 1), ('rs', 'm', 2, 0, 'f'),
    ),
    6: (
        ('rs', 'm', 3, 1, 'n'),
    ),
    7: (
        ('fin', 'e', 1, 0),
    ),
    9: (
        ('rs', 'm', 3, 0, 'f'), ('rs', 'm', 2, 1, 'f'),
    ),
    12: (
        ('ag', 'm', 'n', 0, 0),
    ),
    13: (
        ('fin', 'e', 3, 0),
    ),
    16: (
        ('fin', 'e', 2, 1), ('fin', 'e', 2, 0), ('rs', 'm', 3, 1, 'f'),
    ),
    18: (
        ('ag', 'm', 'n', 0, 1), ('ag', 'm', 'f', 0, 0), ('ag', 'm', 'n', 1, 0),
    ),
    19: (
        ('ag', 'm', 'f', 0, 1), ('ag', 'm', 'n', 1, 1), ('ag', 'm', 'f', 1, 0),
    ),
    20: (
        ('ag', 'm', 'n', 2, 0), ('ag', 'm', 'f', 1, 1), ('ag', 'm', 'n', 2, 1),
    ),
    23: (
        ('fin', 'e', 3, 1), ('ag', 'm', 'f', 2, 0), ('ag', 'm', 'n', 3, 0),
    ),
    25: (
        ('ag', 'e', 'x', 0, 0),
    ),
    27: (
        ('ag', 'm', 'f', 2, 1),
    ),
}
TAIL = (
    ('ag', 'm', 'n', 3, 1), ('ag', 'e', 'x', 2, 1), ('ag', 'e', 'x', 2, 0), ('ag', 'e', 'x', 1, 1), ('ag', 'm', 'f', 3, 0),
    ('ag', 'm', 'f', 3, 1), ('ag', 'e', 'x', 1, 0), ('ag', 'e', 'x', 3, 0), ('ag', 'e', 'x', 0, 1), ('ag', 'e', 'x', 3, 1),
)


def normalize(x_f32, gain, bias):
    row_mean = jnp.mean(x_f32, axis=-1, keepdims=True)
    centered = x_f32 - row_mean
    variance = jnp.mean(centered * centered, axis=-1, keepdims=True)
    return centered * lax.rsqrt(variance + NORM_EPS) * gain + bias


def add_bf16(*terms):
    return sum(t.astype(F32) for t in terms).astype(BF16)


def layer_kernel(x_any, state_in, gain1, bias1, gain2, bias2, wq_any, wk_any, wv_any, wg_any, wo_any, up_any, down_any, cos_first, sin_first, step_rows,
                 out_any, state_ref, up_all, down_all,
                 wq, wk, wv, wg, wo, x_buf, part, met, own, rs, hid, acc, decay, edge, cos_low, sin_low, cos_rows, sin_rows,
                 load_sem, x_sem, mid_sem, state_sem, tile_sem, met_s, met_r, credit, rs_s, rs_r, z_s, z_r, f_s, f_r, g_s, g_r, p_s, p_r, ag_s, ag_r, agp_s, agp_r, put_sem):
    group, me = lax.axis_index('dp'), lax.axis_index('tp')
    chip, core = lax.div(me, 2), lax.rem(me, 2)
    partner = me + 1 - 2 * core
    across_x = lax.rem(group + 2, 4)
    across_y = group + 1 - 2 * lax.rem(group, 2)
    chunk = decay.shape[0]
    rows, share = own.shape[1], rs.shape[2]
    key_dim, half = wq.shape[1], wq.shape[1] // 2
    last = CHIPS - 1
    far = 1 - 2 * lax.div(chip, 2)
    is_end = (chip == 0) | (chip == last)
    is_middle = (chip > 0) & (chip < last)

    def remote(src, dst, s, r, **where):
        return pltpu.make_async_remote_copy(src_ref=src, dst_ref=dst, send_sem=s, recv_sem=r, device_id=where, device_id_type=MESH)

    def side_of(flow):
        return lax.div(1 - flow, 2)

    shard, kept = lax.div(chip, 2), side_of(far)
    weight_all, weight_own = (up_all, down_all), (up_any, down_any)
    quarter = tuple(w.shape[0] // 4 for w in weight_own)

    def origin_of(which):
        return {'n1': chip - far, 'f1': chip + far, 'f2': chip + 2 * far}[which] if isinstance(which, str) else chip + which * far

    def piece(p, index, q):
        return weight_all[p].at[index, pl.ds(q * quarter[p], quarter[p])]

    def z_copy(flow, origin, p, own_piece=False):
        slot = piece(p, 2 * origin + core, group)
        src = weight_own[p].at[pl.ds(group * quarter[p], quarter[p])] if own_piece else slot
        return remote(src, slot, z_s.at[side_of(flow), origin, p], z_r.at[origin, p], tp=me + 2 * flow)

    def first_copy(axis, origin, p, q=None):
        slot = piece(p, 2 * origin + core, group if q is None else q)
        return remote(slot, slot, f_s.at[axis, origin, p], f_r.at[axis, origin, p], dp=across_x if axis == 0 else across_y)

    def second_copy(origin, p, q=None):
        slot = piece(p, 2 * origin + core, (across_x if p == 0 else across_y) if q is None else q)
        return remote(slot, slot, g_s.at[origin, p], g_r.at[origin, p], dp=across_y if p == 0 else across_x)

    def partner_copy(origin, p, own_shard=False, incoming=False):
        slot = weight_all[p].at[2 * origin + (1 - core if incoming else core)]
        return remote(weight_own[p] if own_shard else slot, slot, p_s.at[origin, p], p_r.at[origin, p], tp=partner)

    def spread_first(which, p):
        origin = origin_of(which)
        z_copy(far, origin, p).wait_recv()
        if isinstance(which, str):
            z_copy(far if which == 'n1' else -far, origin, p).start()
        else:
            for axis in range(2):
                first_copy(axis, origin, p).start()

    def spread_second(which, p):
        origin = origin_of(which)
        first_copy(p, origin, p, across_x if p == 0 else across_y).wait_recv()
        second_copy(origin, p).start()

    def spread_third(which, p):
        origin = origin_of(which)
        first_copy(1 - p, origin, p, across_y if p == 0 else across_x).wait_recv()
        second_copy(origin, p, 3 - group).wait_recv()
        partner_copy(origin, p).start()

    def strip(h):
        return pl.ds(h * (share // PARTS), share // PARTS)

    def mine(i, h, side):
        return own[i, pl.ds(pl.multiple_of((1 - side) * share + h * (share // PARTS), share // PARTS), share // PARTS)]

    def rs_copy(flow, i, h, fresh=False):
        side = side_of(flow)
        slot = rs.at[side, i, strip(h)]
        src = own.at[i, pl.ds((1 - side) * share + h * (share // PARTS), share // PARTS)] if fresh else slot
        return remote(src, slot, rs_s.at[side, i, h], rs_r.at[side, i, h], tp=me + 2 * flow)

    def rs_first(i):
        @pl.when(is_end)
        def _():
            for h in range(PARTS):
                rs_copy(far, i, h, fresh=True).start()

    def rs_step(i, h, which):
        flow = far if which == 'n' else -far
        side = side_of(flow)
        rs_copy(flow, i, h).wait_recv()
        rs[side, i, strip(h)] = add_bf16(rs[side, i, strip(h)], mine(i, h, side))
        rs_copy(flow, i, h).start()

    def rs_final(i, h):
        side = side_of(-far)
        rs_copy(-far, i, h).wait_recv()
        rs[kept, i, strip(h)] = add_bf16(rs[kept, i, strip(h)], add_bf16(mine(i, h, side), rs[side, i, strip(h)]))

    def ag_copy(b, h, origin, fresh=False):
        slot = out_any.at[core, b, origin, strip(h)]
        return remote(rs.at[kept, b, strip(h)] if fresh else slot, slot, ag_s.at[b, h, origin], ag_r.at[b, h, origin], tp=me + 2 * (1 - 2 * origin))

    def agp_copy(b, h, origin, fresh=False, incoming=False):
        slot = out_any.at[1 - core if incoming else core, b, origin, strip(h)]
        return remote(rs.at[kept, b, strip(h)] if fresh else slot, slot, agp_s.at[b, h, origin], agp_r.at[b, h, origin], tp=partner)

    def put_copy(b):
        return pltpu.make_async_copy(rs.at[kept, b], out_any.at[core, b, shard], put_sem.at[b])

    def ag_first(b):
        for h in range(PARTS):
            ag_copy(b, h, shard, fresh=True).start()
        for h in range(PARTS):
            agp_copy(b, h, shard, fresh=True).start()
        put_copy(b).start()

    def ag_step(which, b, h):
        origin = shard if which == 'n' else 1 - shard
        ag_copy(b, h, origin).wait_recv()
        if which != 'x':
            ag_copy(b, h, origin).start()
        agp_copy(b, h, origin).start()

    serves = {'s1': spread_first, 's2': spread_second, 's3': spread_third, 'rs': rs_step, 'fin': rs_final, 'ag': ag_step}

    def serve(items):
        for item in items:
            @pl.when(is_end if item[1] == 'e' else is_middle)
            def _():
                serves[item[0]](*item[2:])

    def x_copy(n):
        seq = core + (1 - 2 * core) * (1 - lax.rem(n, 2))
        return pltpu.make_async_copy(x_any.at[seq, lax.div(n, 2)], x_buf, x_sem)

    def met_copy():
        return remote(part, met, met_s, met_r, tp=partner)

    barrier = pltpu.get_barrier_semaphore()
    for where in ({'tp': partner}, {'dp': across_x}, {'dp': across_y}):
        pl.semaphore_signal(barrier, inc=1, device_id=where, device_id_type=MESH)

    @pl.when(chip < last)
    def _():
        pl.semaphore_signal(barrier, inc=1, device_id={'tp': me + 2}, device_id_type=MESH)

    @pl.when(chip > 0)
    def _():
        pl.semaphore_signal(barrier, inc=1, device_id={'tp': me - 2}, device_id_type=MESH)

    loads = [pltpu.make_async_copy(a, b, load_sem.at[k]) for k, (a, b) in enumerate(((wq_any, wq), (wk_any, wk), (wv_any, wv), (wg_any, wg), (wo_any, wo)))]
    x_copy(0).start()
    for load in loads:
        load.start()
    state_load = pltpu.make_async_copy(state_in, state_ref, state_sem)
    state_load.start()
    mid_load = pltpu.make_async_copy(x_any.at[core, :, shard], rs.at[kept], mid_sem)

    @pl.when(is_end)
    def _():
        mid_load.start()

    pl.semaphore_wait(barrier, 4 + is_middle.astype(jnp.int32))

    for p in range(2):
        z_copy(far, chip, p, own_piece=True).start()

        @pl.when(is_middle)
        def _():
            z_copy(-far, chip, p, own_piece=True).start()

        @pl.when(is_end)
        def _():
            partner_copy(chip, p, own_shard=True).start()

    log_gamma = F32(0.0)
    for head in range(2 * CHIPS):
        log_gamma = jnp.where(me == head, F32(math.log1p(-2.0 ** (-5 - head))), log_gamma)
    gap = lax.broadcasted_iota(jnp.int32, (chunk, chunk), 0) - lax.broadcasted_iota(jnp.int32, (chunk, chunk), 1)
    decay[...] = jnp.where(gap >= 0, jnp.exp(jnp.maximum(gap, 0).astype(F32) * log_gamma), 0.0)
    lane = lax.broadcasted_iota(jnp.int32, edge.shape, 1)
    ids = lax.broadcasted_iota(jnp.int32, edge.shape, 0)
    power = jnp.where(lane == 0, ids + 1, jnp.where(lane == 1, chunk - 1 - ids, chunk))
    edge[...] = jnp.exp(power.astype(F32) * log_gamma)
    turns = chunk // LOW
    cos_b, sin_b = step_rows[0, turns:turns + LOW, :], step_rows[1, turns:turns + LOW, :]
    for turn in range(turns):
        span = slice(turn * LOW, (turn + 1) * LOW)
        cos_a, sin_a = step_rows[0, turn:turn + 1, :], step_rows[1, turn:turn + 1, :]
        cos_low[span, :] = cos_a * cos_b - sin_a * sin_b
        sin_low[span, :] = sin_a * cos_b + cos_a * sin_b
    cos_b, sin_b = step_rows[0, turns + LOW:, :], step_rows[1, turns + LOW:, :]
    for seq in range(2):
        span = slice(seq * cos_b.shape[0], (seq + 1) * cos_b.shape[0])
        cos_a, sin_a = cos_first[seq:seq + 1, :], sin_first[seq:seq + 1, :]
        cos_rows[span, :] = cos_a * cos_b - sin_a * sin_b
        sin_rows[span, :] = sin_a * cos_b + cos_a * sin_b
    for load in loads:
        load.wait()
    state_load.wait()

    @pl.when(is_end)
    def _():
        mid_load.wait()


    def attend(n, carry):
        i, k = lax.div(n, 2), lax.rem(n, 2)
        seq = core + (1 - 2 * core) * (1 - k)
        x_copy(n).wait()

        h = normalize(x_buf[...].reshape(rows, part.shape[1]).astype(F32), gain1[...], bias1[...]).astype(BF16)

        @pl.when(n < 2 * BLOCKS - 1)
        def _():
            x_copy(n + 1).start()

        q_raw = jnp.dot(h, wq[...], preferred_element_type=F32)
        k_raw = jnp.dot(h, wk[...], preferred_element_type=F32)
        v_all = jnp.dot(h, wv[...], preferred_element_type=F32).astype(BF16)
        g_all = jnp.dot(h, wg[...], preferred_element_type=F32)
        cos_lo, sin_lo = cos_low[...], sin_low[...]
        mixed = []
        subs = rows // chunk
        for sub in range(subs):
            span = slice(sub * chunk, (sub + 1) * chunk)
            row = pl.ds(seq * (BLOCKS * subs) + i * subs + sub, 1)
            cos_hi, sin_hi = cos_rows[row, :], sin_rows[row, :]
            cos_t = cos_hi * cos_lo - sin_hi * sin_lo
            sin_t = sin_hi * cos_lo + cos_hi * sin_lo

            def rotate(raw):
                first, second = raw[span, :half], raw[span, half:]
                return jnp.concatenate([first * cos_t - second * sin_t, second * cos_t + first * sin_t], axis=-1)

            queries = rotate(q_raw).astype(BF16)
            keys = (rotate(k_raw) * key_dim ** -0.5).astype(BF16)
            values = v_all[span]
            state = state_ref[seq, 0]
            scores = lax.dot_general(queries, keys, (((1,), (1,)), ((), ())), preferred_element_type=F32) * decay[...]
            retained = jnp.dot(scores.astype(BF16), values, preferred_element_type=F32)
            retained += jnp.dot(queries, state.astype(BF16), preferred_element_type=F32) * edge[:, 0:1]
            keys_decayed = (keys.astype(F32) * edge[:, 1:2]).astype(BF16)
            grown = lax.dot_general(keys_decayed, values, (((0,), (0,)), ((), ())), preferred_element_type=F32)
            state_ref[seq, 0] = state * edge[0:1, 2:3] + grown
            row_mean = jnp.mean(retained, axis=-1, keepdims=True)
            centered = retained - row_mean
            variance = jnp.mean(centered * centered, axis=-1, keepdims=True)
            normed = centered * lax.rsqrt(variance + GROUP_EPS)
            mixed.append((jax.nn.silu(g_all[span]) * normed).astype(BF16))
        u = jnp.dot(jnp.concatenate(mixed, axis=0), wo[...], preferred_element_type=F32).astype(BF16)

        @pl.when(k == 1)
        def _():
            met_copy().wait_send()

        part[...] = u

        @pl.when(k == 0)
        def _():
            @pl.when(i >= 1)
            def _():
                pl.semaphore_wait(credit, 1)

            met_copy().start()

        @pl.when(k == 1)
        def _():
            met_copy().wait_recv()
            own[i] = add_bf16(part[...], met[...])

            @pl.when(i < BLOCKS - 1)
            def _():
                pl.semaphore_signal(credit, inc=1, device_id={'tp': partner}, device_id_type=MESH)

            rs_first(i)

        for turn, items in LOOP.items():
            @pl.when(n == turn)
            def _():
                serve(items)

        return carry

    lax.fori_loop(0, 2 * BLOCKS, attend, 0)

    serve(BETWEEN)

    slots = ((wv, wo), (wg, part))

    def tile_copies(index, slot, own_shard=False):
        sources = (up_any, down_any) if own_shard else (up_all.at[index], down_all.at[index])
        return [pltpu.make_async_copy(sources[p], slots[slot][p], tile_sem.at[slot, p]) for p in range(2)]

    def ffn_tile(slot):
        for copy in tile_copies(0, slot):
            copy.wait()
        up, down = slots[slot]
        pre = jnp.dot(hid[...], up[...], preferred_element_type=F32)
        act = (0.5 * pre * (1.0 + lax.erf(pre * 0.5 ** 0.5))).astype(BF16)
        acc[...] += jnp.dot(act, down[...], preferred_element_type=F32)

    def ffn_finish(b):
        rs[kept, b] = add_bf16(rs[kept, b], acc[...].astype(BF16))
        ag_first(b)

    def serve_at(pair, parity, fresh):
        for turn, items in TILES.items():
            if turn % 2 == parity and (turn % 8 == 0) == fresh:
                @pl.when(pair == turn // 2)
                def _():
                    serve(items)

    def ffn_pair(pair, carry):
        b, e = lax.div(pair, CHIPS), lax.rem(pair, CHIPS)
        index = 2 * (chip + e * far) + core
        serve_at(pair, 0, False)

        @pl.when(is_end)
        def _():
            @pl.when(e == 0)
            def _():
                for copy in tile_copies(index, 0, own_shard=True):
                    copy.start()

            @pl.when(e > 0)
            def _():
                for copy in tile_copies(index, 0):
                    copy.start()

            @pl.when(pair > 0)
            def _():
                ffn_tile(1)

                @pl.when(e == 0)
                def _():
                    ffn_finish(b - 1)

        serve_at(pair, 0, True)

        @pl.when(is_end & (e == 0))
        def _():
            hid[...] = normalize(rs[kept, b].astype(F32), gain2[...], bias2[...]).astype(BF16)
            acc[...] = jnp.zeros_like(acc)

        serve_at(pair, 1, False)

        @pl.when(is_end)
        def _():
            @pl.when(b == 0)
            def _():
                for p in range(2):
                    partner_copy(chip + e * far, p, incoming=True).wait_recv()

            for copy in tile_copies(index + 1 - 2 * core, 1):
                copy.start()
            ffn_tile(0)

        return carry

    lax.fori_loop(0, BLOCKS * CHIPS, ffn_pair, 0)

    @pl.when(is_end)
    def _():
        ffn_tile(1)
        ffn_finish(BLOCKS - 1)

    serve(TAIL)

    strips = [(b, h) for b in range(BLOCKS) for h in range(PARTS)]
    for b, h in strips:
        for origin in range(2):
            agp_copy(b, h, origin).wait_send()
            agp_copy(b, h, origin, incoming=True).wait_recv()
    for p in range(2):
        z_copy(far, chip, p).wait_send()

    @pl.when(is_end)
    def _():
        for b in range(BLOCKS):
            put_copy(b).wait()
        for b, h in strips:
            ag_copy(b, h, shard).wait_send()
            rs_copy(far, b, h, fresh=True).wait_send()
        for p in range(2):
            partner_copy(chip, p, own_shard=True).wait_send()
            for which in range(1, CHIPS):
                origin = origin_of(which)
                partner_copy(origin, p).wait_send()
                second_copy(origin, p).wait_send()
                for axis in range(2):
                    first_copy(axis, origin, p).wait_send()

    @pl.when(is_middle)
    def _():
        for p in range(2):
            z_copy(-far, chip, p).wait_send()
            z_copy(far, origin_of('n1'), p).wait_send()
            z_copy(-far, origin_of('f1'), p).wait_send()
            z_copy(-far, origin_of('f2'), p).wait_send()
        for b, h in strips:
            for side in range(2):
                rs_copy(1 - 2 * side, b, h).wait_send()
                ag_copy(b, h, side).wait_send()


def solution(mesh):
    members = mesh.shape['tp']

    def local_layer(x_in, start_pos, kv_state, ln1_gain, ln1_bias, w_q, w_k, w_v, w_g, w_o, ln2_gain, ln2_bias, w_up, w_down):
        seqs, chunk_len, d_model = x_in.shape
        key_dim = kv_state.shape[2]
        half = key_dim // 2
        rows = chunk_len // BLOCKS
        share = rows // 2
        chunk = min(CHUNK, rows)
        inv_freq = (ROPE_BASE ** (-np.arange(half) / half)).astype(np.float32)
        angles = start_pos.astype(F32)[:, None] * inv_freq[None, :]
        steps = np.concatenate([np.arange(0, chunk, LOW), np.arange(LOW), np.arange(0, chunk_len, chunk)])
        turns = steps[:, None] * inv_freq.astype(np.float64)
        step_rows = jnp.asarray(np.stack([np.cos(turns), np.sin(turns)]).astype(np.float32))

        anywhere = pl.BlockSpec(memory_space=pl.ANY)
        vmem = pl.BlockSpec(memory_space=pltpu.VMEM)
        dma = lambda *shape: pltpu.SemaphoreType.DMA(shape)
        out, state, _, _ = pl.pallas_call(
            layer_kernel,
            in_specs=[anywhere, anywhere, vmem, vmem, vmem, vmem] + [anywhere] * 7 + [vmem] * 3,
            out_specs=[anywhere, vmem, anywhere, anywhere],
            out_shape=[
                pltpu.VMEM((seqs, BLOCKS, 2, share, d_model), BF16),
                jax.ShapeDtypeStruct(kv_state.shape, F32),
                jax.ShapeDtypeStruct((members,) + w_up.shape, BF16),
                jax.ShapeDtypeStruct((members,) + w_down.shape, BF16),
            ],
            scratch_shapes=[
                pltpu.VMEM(w_q.shape, BF16), pltpu.VMEM(w_k.shape, BF16), pltpu.VMEM(w_v.shape, BF16), pltpu.VMEM(w_g.shape, BF16),
                pltpu.VMEM(w_o.shape, BF16),
                pltpu.VMEM((2, share, d_model), BF16), pltpu.VMEM((rows, d_model), BF16), pltpu.VMEM((rows, d_model), BF16),
                pltpu.VMEM((BLOCKS, rows, d_model), BF16), pltpu.VMEM((2, BLOCKS, share, d_model), BF16),
                pltpu.VMEM((share, d_model), BF16), pltpu.VMEM((share, d_model), F32),
                pltpu.VMEM((chunk, chunk), F32), pltpu.VMEM((chunk, 128), F32), *[pltpu.VMEM((count, half), F32) for count in (chunk, chunk, seqs * (chunk_len // chunk), seqs * (chunk_len // chunk))],
                dma(5), pltpu.SemaphoreType.DMA, pltpu.SemaphoreType.DMA, pltpu.SemaphoreType.DMA, dma(2, 2), pltpu.SemaphoreType.DMA, pltpu.SemaphoreType.DMA, pltpu.SemaphoreType.REGULAR,
                dma(2, BLOCKS, PARTS), dma(2, BLOCKS, PARTS), dma(2, 4, 2), dma(4, 2), dma(2, 4, 2), dma(2, 4, 2), dma(4, 2), dma(4, 2), dma(4, 2), dma(4, 2),
                dma(BLOCKS, PARTS, 2), dma(BLOCKS, PARTS, 2), dma(BLOCKS, PARTS, 2), dma(BLOCKS, PARTS, 2), dma(BLOCKS),
            ],
            compiler_params=pltpu.CompilerParams(collective_id=0, has_side_effects=True, vmem_limit_bytes=47 * 2 ** 20),
            name="layer",
        )(x_in.reshape(seqs, BLOCKS, 2, share, d_model), kv_state, *(a[None, :] for a in (ln1_gain, ln1_bias, ln2_gain, ln2_bias)), w_q, w_k, w_v, w_g, w_o, w_up, w_down, jnp.cos(angles), jnp.sin(angles), step_rows)
        return out.reshape(seqs, chunk_len, d_model), state

    in_specs = (P('dp', None, None), P('dp'), P('dp', 'tp', None, None), P(), P(), P(None, 'tp'), P(None, 'tp'), P(None, 'tp'), P(None, 'tp'), P('tp', None), P(), P(), P(None, 'tp'), P('tp', None))
    out_specs = (P('dp', None, None), P('dp', 'tp', None, None))
    return jax.shard_map(local_layer, mesh=mesh, in_specs=in_specs, out_specs=out_specs, check_vma=False)
```
